32 devices in a mesh: dom: 8 (over z, x), sub: 4 (over y, core).
Axes of the slice: x: 2, y: 2, z: 4, core: 2. Of those that a mesh axis runs over, the one named last changes fastest.
Arguments:
- features: bfloat16 [32768, 256], P(('dom', 'sub')), may hold values from -16 to 16
- weight: bfloat16 [256, 256], replicated, may hold values from -0.375 to 0.375
- send_far: int32 [16384], P(('dom', 'sub')), may hold values from 0 to 1023
- send_near: int32 [4096], P(('dom', 'sub')), may hold values from 0 to 1023
- tile_dst: int32 [512], P(('dom', 'sub')), may hold values from 0 to 7
- inner_src: int32 [256], P(('dom', 'sub')), may hold values from 0 to 7
- outer_src: int32 [256], P(('dom', 'sub')), may hold values from 0 to 4
- tile_live: int32 [32, 2], P(('dom', 'sub')), may hold values from 4 to 8
- tile_weight: bfloat16 [512, 128, 128], P(('dom', 'sub')), may hold values from -0.3125 to 0.3125
Outputs:
- whitened: bfloat16 [32768, 256], P(('dom', 'sub'))
- loss_value: float32 [], replicated
The draws below stay inside these ranges and needn't reach their ends.
Inputs may be any that keep to these rules, and one draw needn't show every extreme that they name: `send_far`: rows may repeat. `tile_live`: live slots come first in each half of a device's slots.
All inputs are finite; a program needn't handle non-finite values.
Results may differ from the reference program's by a relative error of at most 0.0085.
Values may be sent and summed in bfloat16 or wider, within the bound.
A program may use at most 64 MiB of HBM per device.

```python
import jax
import jax.numpy as jnp
from jax import lax

F = 256
B = 128
V_DEV = 1024
HALO_DOM = 512
SLOTS = 8
HALO_SUB = 128
PEER_DOM = 64
PEER_SUB = 32
VERTS = 32768
N_DOM = 8
N_SUB = 4


def draw_features(key, part):
    key_base = jax.random.fold_in(key, 11)
    key_jitter = jax.random.fold_in(key, 14)
    key_shift = jax.random.fold_in(key, 15)
    key_heavy = jax.random.fold_in(key, 16)
    key_sign = jax.random.fold_in(key, 17)
    block_count = VERTS // V_DEV
    block_index = jnp.arange(block_count, dtype=jnp.int32)
    sub_place = (block_index % N_SUB).astype(jnp.float32) / max(N_SUB - 1, 1)
    dom_place = (block_index // N_SUB).astype(jnp.float32) / max(block_count // N_SUB - 1, 1)
    jitter = jax.random.uniform(key_jitter, (block_count,), jnp.float32, -0.3, 0.3)
    block_scale = jnp.exp(-0.6 + 0.6 * sub_place + 0.5 * dom_place + jitter)
    block_shift = jax.random.uniform(key_shift, (block_count, 1, F), jnp.float32, -0.5, 0.5)
    array_shape = (block_count, V_DEV, F)
    base_values = jnp.clip(jax.random.normal(key_base, array_shape, jnp.float32), -6.0, 6.0)
    values = base_values * block_scale[:, None, None] + block_shift
    values = jnp.clip(values, -9.0, 9.0)
    heavy_noise = jnp.clip(jax.random.normal(key_heavy, (block_count, V_DEV, 1), jnp.float32), -2.5, 2.5)
    block_sign = jnp.where(jax.random.bernoulli(key_sign, 0.5, (block_count, 1, 1)), 1.0, -1.0).astype(jnp.float32)
    heavy_values = block_sign * (12.0 + 1.5 * heavy_noise)
    column_index = jnp.arange(F, dtype=jnp.int32)
    heavy_mask = column_index[None, None, :] == (block_index % F)[:, None, None]
    values = jnp.where(heavy_mask, heavy_values, values)
    values = jnp.clip(values, -16.0, 16.0).reshape(VERTS, F)
    return values.astype(jnp.bfloat16)


def plant(entries, own_key, least, top_value):
    longest = entries.shape.index(max(entries.shape))
    spots = []
    for shift in (0, 1):
        where = [jax.random.randint(jax.random.fold_in(own_key, axis), (), 0, length) for axis, length in enumerate(entries.shape)]
        where[longest] = (where[longest] + shift) % entries.shape[longest]
        spots.append(tuple(where))
    return entries.at[spots[0]].set(least).at[spots[1]].set(top_value)


def steps_of(stream_key, shape, cuts, low, top_value):
    def one(dim, parts):
        heights = jax.random.uniform(jax.random.fold_in(jax.random.fold_in(stream_key, 6), dim), (parts,), jnp.float32, low / len(cuts), top_value / len(cuts))
        return jnp.repeat(jnp.exp(heights), shape[dim] // parts).reshape((-1,) + (1,) * (len(shape) - dim - 1))

    loudness = one(*cuts[0])
    for cut in cuts[1:]:
        loudness = loudness * one(*cut)
    return loudness


def normal_values(key, extent, deviation, limit, pieces=(), kind=jnp.bfloat16):
    level = steps_of(key, extent, pieces, -0.22, 0.18) if pieces else 1.0
    result = jax.random.normal(key, extent, jnp.float32) * deviation * level
    return jnp.minimum(jnp.maximum(result, -limit), limit).astype(kind)


def setup_inputs(seed: int = 0) -> dict:
    key_of = jax.random.split(jax.random.key(seed), 10)
    return {
        "features": draw_features(jax.random.fold_in(key_of[9], 71), 0),
        "weight": normal_values(key_of[1], (F, F), F ** -0.5, 0.375),
        "send_far": plant(jax.random.randint(key_of[2], (N_DOM * N_SUB * HALO_DOM,), 0, V_DEV), jax.random.fold_in(key_of[2], 1), 0, V_DEV - 1).astype(jnp.int32),
        "send_near": plant(jax.random.randint(key_of[3], (N_DOM * N_SUB * HALO_SUB,), 0, V_DEV), jax.random.fold_in(key_of[3], 1), 0, V_DEV - 1).astype(jnp.int32),
        "tile_dst": plant(jax.random.randint(key_of[4], (N_DOM * N_SUB * 2 * SLOTS,), 0, V_DEV // B), jax.random.fold_in(key_of[4], 1), 0, (V_DEV // B) - 1).astype(jnp.int32),
        "inner_src": plant(jax.random.randint(key_of[5], (N_DOM * N_SUB * SLOTS,), 0, V_DEV // B), jax.random.fold_in(key_of[5], 1), 0, (V_DEV // B) - 1).astype(jnp.int32),
        "outer_src": plant(jax.random.randint(key_of[6], (N_DOM * N_SUB * SLOTS,), 0, (HALO_DOM + HALO_SUB) // B), jax.random.fold_in(key_of[6], 1), 0, ((HALO_DOM + HALO_SUB) // B) - 1).astype(jnp.int32),
        "tile_live": plant(jax.random.randint(key_of[7], (N_DOM * N_SUB, 2), SLOTS // 2, SLOTS + 1), jax.random.fold_in(key_of[7], 1), SLOTS // 2, SLOTS).astype(jnp.int32),
        "tile_weight": normal_values(key_of[8], (N_DOM * N_SUB * 2 * SLOTS, B, B), (3 * B) ** -0.5, 0.3125, ((0, 32),)),
    }


epsilon = 1e-05

def whiten_map(gram_sum, vertex_count, feat_width):
    identity = jnp.eye(feat_width, dtype=jnp.float32)
    scaled = gram_sum / vertex_count + epsilon * identity
    lower = jnp.linalg.cholesky(scaled)
    inverse = lax.linalg.triangular_solve(lower, identity, left_side=True, lower=True)
    return inverse.T

def reference(features, weight, send_far, send_near, tile_dst, inner_src, outer_src, tile_live, tile_weight):
    device_total = N_DOM * N_SUB
    local_tiles = V_DEV // B
    blocks = features.reshape(N_DOM, N_SUB, V_DEV, F)
    far_lists = send_far.reshape(N_DOM, N_SUB, N_DOM, PEER_DOM)
    near_lists = send_near.reshape(N_DOM, N_SUB, N_SUB, PEER_SUB)
    dest_tiles = tile_dst.reshape(device_total, 2 * SLOTS)
    inner_tiles = inner_src.reshape(device_total, SLOTS)
    outer_tiles = outer_src.reshape(device_total, SLOTS)
    slot_weights = tile_weight.reshape(device_total, 2 * SLOTS, B, B)

    def per_device(device_index):
        dom_index = device_index // N_SUB
        sub_index = device_index % N_SUB
        same_sub = blocks[:, sub_index]
        far_index = far_lists[:, sub_index, dom_index, :]
        far_rows = jnp.take_along_axis(same_sub, far_index[:, :, None], axis=1).reshape(HALO_DOM, F)
        same_dom = blocks[dom_index]
        near_index = near_lists[dom_index, :, sub_index, :]
        near_rows = jnp.take_along_axis(same_dom, near_index[:, :, None], axis=1).reshape(HALO_SUB, F)
        own_rows = blocks[dom_index, sub_index]
        tile_table = jnp.concatenate([own_rows, far_rows, near_rows], 0).reshape(-1, B, F).astype(jnp.float32)
        source_tiles = jnp.concatenate([inner_tiles[device_index], outer_tiles[device_index] + local_tiles])
        selected = tile_table[source_tiles]
        products = jnp.einsum('kij,kjf->kif', slot_weights[device_index].astype(jnp.float32), selected, precision=lax.Precision.HIGHEST)
        slot_index = jnp.arange(SLOTS, dtype=jnp.int32)
        slot_mask = jnp.concatenate([slot_index < tile_live[device_index, 0], slot_index < tile_live[device_index, 1]])
        tile_index = jnp.arange(local_tiles, dtype=jnp.int32)
        selector = ((dest_tiles[device_index][None, :] == tile_index[:, None]) & slot_mask[None, :]).astype(jnp.float32)
        summed = jnp.einsum('tk,kif->tif', selector, products, precision=lax.Precision.HIGHEST).reshape(V_DEV, F)
        aggregate = summed.astype(jnp.bfloat16)
        projected = jnp.dot(aggregate.astype(jnp.float32), weight.astype(jnp.float32), preferred_element_type=jnp.float32)
        return (own_rows.astype(jnp.float32) + jax.nn.silu(projected)).astype(jnp.bfloat16)
    hidden = lax.map(per_device, jnp.arange(device_total, dtype=jnp.int32)).reshape(VERTS, F)
    gram_sum = lax.dot_general(hidden.astype(jnp.float32), hidden.astype(jnp.float32), (((0,), (0,)), ((), ())), preferred_element_type=jnp.float32)
    whitener = whiten_map(gram_sum, VERTS, F)
    white = jnp.dot(hidden.astype(jnp.float32), whitener, precision=lax.Precision.HIGHEST)
    distance = white - features.astype(jnp.float32)
    loss_value = jnp.sum(distance * distance) / (VERTS * F)
    return (white.astype(jnp.bfloat16), loss_value)
```

```python
import functools

import jax
import jax.numpy as jnp
from jax import lax
from jax.experimental import pallas as pl
from jax.experimental.pallas import tpu as pltpu
from jax.sharding import PartitionSpec as P

epsilon = 1e-05
MESH = pl.DeviceIdType.MESH
LEAF = 64
HIGH = lax.Precision.HIGHEST


def one_hot_rows(index_row, row_count):
    rows = index_row.shape[1]
    columns = jnp.broadcast_to(index_row, (128, rows)).T
    lane = lax.broadcasted_iota(jnp.int32, (rows, 128), 1)
    parts = [
        jnp.where(columns == lane + start, 1.0, 0.0).astype(jnp.bfloat16)
        for start in range(0, row_count, 128)
    ]
    return jnp.concatenate(parts, axis=1)


def padded_rows(count):
    return -(-count // 16) * 16


def packing(packed_rows, padded_total, n_dom, n_sub, per_dom, per_sub, near_rows_each):
    near_total = n_sub * near_rows_each
    far_total = packed_rows - near_total
    far_rows_each = far_total // n_dom
    row = lax.broadcasted_iota(jnp.int32, (packed_rows, padded_total), 0)
    column = lax.broadcasted_iota(jnp.int32, (packed_rows, padded_total), 1)
    far_place = row + lax.div(row, far_rows_each) * (per_dom - far_rows_each)
    near_row = row - far_total
    near_place = (
        n_dom * per_dom + near_row + lax.div(near_row, near_rows_each) * (per_sub - near_rows_each)
    )
    place = jnp.where(row < far_total, far_place, near_place)
    return jnp.where(place == column, 1.0, 0.0).astype(jnp.bfloat16)


def leaf_inverse(block):
    size = block.shape[0]
    row = lax.broadcasted_iota(jnp.int32, (size, size), 0)
    lane = lax.broadcasted_iota(jnp.int32, (size, size), 1)
    work = jnp.concatenate([block, jnp.where(row == lane, 1.0, 0.0)], axis=1)
    group = 8
    done = []
    for step in range(0, size, group):
        lines = [work[i : i + 1, :] for i in range(group)]
        entry = {
            (i, j): jnp.broadcast_to(lines[i][:, step + j : step + j + 1], (1, 2 * size))
            for i in range(group)
            for j in range(i, group)
        }
        inverse = []
        for i in range(group):
            inverse.append(1.0 / entry[i, i])
            for j in range(i + 1, group):
                share = entry[i, j] * inverse[i]
                for k in range(j, group):
                    entry[j, k] = entry[j, k] - share * entry[i, k]
                lines[j] = lines[j] - share * lines[i]
            done.append((lines[i] / jnp.sqrt(entry[i, i]))[:, size:])
        if step + group == size:
            break
        solved = [None] * group
        for i in reversed(range(group)):
            line = lines[i]
            for j in range(i + 1, group):
                line = line - entry[i, j] * solved[j]
            solved[i] = line * inverse[i]
        work = work[group:, :]
        update = work[:, step : step + 1] * solved[0]
        for i in range(1, group):
            update = update + work[:, step + i : step + i + 1] * solved[i]
        work = work - update
    return jnp.concatenate(done, axis=0)


def far_first(index, count, turn):
    if count % 2:
        return lax.rem(index + 1 + turn, count)
    half = count // 2
    mine = lax.div(index, half) * half
    other = half - mine
    return jnp.where(
        turn < half,
        other + lax.rem(index + half // 2 + turn, half),
        mine + lax.rem(index + 1 + turn, half),
    )


def kernel(
    n_dom,
    n_sub,
    near_each,
    features_in,
    weight_in,
    far_in,
    near_in,
    dst_in,
    inner_in,
    outer_in,
    live_in,
    tile_in,
    out_ref,
    loss_ref,
    features_ref,
    weight_ref,
    far_ref,
    near_ref,
    dst_ref,
    inner_ref,
    outer_ref,
    live_ref,
    tile_ref,
    result,
    far_send,
    near_send,
    arrived,
    table,
    products,
    acc,
    aggregate,
    features_t,
    part,
    part_in,
    part_own,
    whole,
    work,
    load_sems,
    halo_sems,
    sum_sems,
):
    total_devices = n_dom * n_sub
    dom = lax.axis_index("dom")
    sub = lax.axis_index("sub")
    me = dom * n_sub + sub
    tiles, size, feat = features_ref.shape
    rows = tiles * size
    slots = inner_ref.shape[0]
    share = part_own.shape[1]
    owners = part.shape[1] // share
    first_owner = (total_devices - owners) // 2
    mine = me - first_owner
    owns = jnp.logical_and(mine >= 0, mine < owners)

    def share_rows(owner):
        return pl.ds(pl.multiple_of(owner * share, share), share)

    def device_of(index):
        return (lax.div(index, n_sub), lax.rem(index, n_sub))

    incoming = (
        (far_in, far_ref),
        (near_in, near_ref),
        (features_in, features_ref),
        (inner_in, inner_ref),
        (outer_in, outer_ref),
        (dst_in, dst_ref),
        (live_in, live_ref),
        (tile_in, tile_ref),
        (weight_in, weight_ref),
    )
    loads = [
        pltpu.make_async_copy(source, target, load_sems.at[place])
        for place, (source, target) in enumerate(incoming)
    ]

    barrier = pltpu.get_barrier_semaphore()

    @pl.loop(1, total_devices)
    def _(offset):
        peer = lax.rem(me + offset, total_devices)
        pl.semaphore_signal(barrier, inc=1, device_id=device_of(peer), device_id_type=MESH)

    for load in loads:
        load.start()
    for load in loads[:3]:
        load.wait()

    features = features_ref[...].reshape(rows, feat)
    far_rows = jnp.dot(
        one_hot_rows(far_ref[...], rows), features, preferred_element_type=jnp.float32
    ).astype(jnp.bfloat16)
    near_rows = jnp.dot(
        one_hot_rows(near_ref[...], rows), features, preferred_element_type=jnp.float32
    ).astype(jnp.bfloat16)
    far_send[...] = far_rows
    near_send[...] = near_rows
    per_dom = far_send.shape[0] // n_dom
    per_sub = near_send.shape[0] // n_sub
    far_count = per_dom * n_dom
    packed = size % per_dom == 0 and size % per_sub == 0 and arrived.shape[0] == table.shape[0] * size

    def place(first, count):
        if packed:
            within = pl.multiple_of(lax.rem(first, size), count)
            return table.at[lax.div(first, size), pl.ds(within, count)]
        return arrived.at[pl.ds(pl.multiple_of(first, count), count)]

    def dom_rows(index):
        return pl.ds(pl.multiple_of(index * per_dom, per_dom), per_dom)

    def sub_rows(index):
        return pl.ds(pl.multiple_of(index * per_sub, per_sub), per_sub)

    def dom_place(index):
        return place(index * per_dom, per_dom)

    def sub_place(index):
        return place(far_count + index * per_sub, per_sub)

    pl.semaphore_wait(barrier, total_devices - 1)

    @pl.loop(0, n_dom - 1)
    def _(turn):
        peer = far_first(dom, n_dom, turn)
        pltpu.make_async_remote_copy(
            src_ref=far_send.at[dom_rows(peer)],
            dst_ref=dom_place(dom),
            send_sem=halo_sems.at[0],
            recv_sem=halo_sems.at[1],
            device_id=(peer, sub),
            device_id_type=MESH,
        ).start()

    @pl.loop(0, n_sub - 1)
    def _(turn):
        peer = far_first(sub, n_sub, turn)
        pltpu.make_async_remote_copy(
            src_ref=near_send.at[sub_rows(peer)],
            dst_ref=sub_place(sub),
            send_sem=halo_sems.at[2],
            recv_sem=halo_sems.at[3],
            device_id=(dom, peer),
            device_id_type=MESH,
        ).start()

    dom_place(dom)[...] = far_send[dom_rows(dom), :]
    sub_place(sub)[...] = near_send[sub_rows(sub), :]

    def slot_products(rows_ref, source, first):
        for slot in range(slots):
            products[slot] = jnp.dot(
                tile_ref[first + slot],
                rows_ref[source[slot]],
                preferred_element_type=jnp.float32,
            )

    def slot_sum(tile, first, count):
        total = None
        for slot in range(slots):
            target = jnp.full((1, feat), dst_ref[first + slot], jnp.int32)
            chosen = jnp.where(jnp.logical_and(target == tile, count > slot), 1.0, 0.0)
            term = products[slot] * chosen
            total = term if total is None else total + term
        return total

    for load in loads[3:]:
        load.wait()
    slot_products(features_ref, inner_ref, 0)
    features_t[...] = features.T
    squares = features.astype(jnp.float32)
    squares = jnp.sum(squares * squares, axis=0, keepdims=True)
    square_row = squares[:, :128]
    for side in range(128, feat, 128):
        square_row = square_row + squares[:, side : side + 128]
    inner_count = jnp.full((1, feat), live_ref[0, 0], jnp.int32)
    outer_count = jnp.full((1, feat), live_ref[0, 1], jnp.int32)

    @pl.loop(0, tiles)
    def _(tile):
        acc[tile] = slot_sum(tile, 0, inner_count)

    def settle(ref, sem):
        pltpu.make_async_copy(ref, ref, sem).wait()

    settle(arrived.at[pl.ds(0, per_dom * (n_dom - 1))], halo_sems.at[1])
    settle(arrived.at[pl.ds(0, per_sub * (n_sub - 1))], halo_sems.at[3])
    if not packed:
        table[...] = jnp.dot(
            packing(table.shape[0] * size, arrived.shape[0], n_dom, n_sub, per_dom, per_sub, near_each),
            arrived[...],
            preferred_element_type=jnp.float32,
        ).astype(jnp.bfloat16).reshape(table.shape)
    slot_products(table, outer_ref, slots)

    @pl.loop(0, tiles)
    def _(tile):
        total = acc[tile] + slot_sum(tile, slots, outer_count)
        aggregate[pl.ds(pl.multiple_of(tile * size, size), size), :] = total.astype(jnp.bfloat16)

    projected = jnp.dot(aggregate[...], weight_ref[...], preferred_element_type=jnp.float32)
    hidden = (
        features_ref[...].reshape(rows, feat).astype(jnp.float32) + projected / (1.0 + jnp.exp(-projected))
    ).astype(jnp.bfloat16)
    hidden_t = hidden.T
    row = lax.broadcasted_iota(jnp.int32, (128, 128), 0)
    lane = lax.broadcasted_iota(jnp.int32, (128, 128), 1)
    tops = range(0, feat, 256)
    sides = [(top, side) for top in range(0, feat, 128) for side in range(top + 128, feat, 128)]
    pair_at = {top: top // 2 for top in tops}
    side_at = {pair: feat // 2 + 128 * place for place, pair in enumerate(sides)}
    extra_at = feat // 2 + 128 * len(sides)

    def diagonal_row(block):
        return jnp.sum(jnp.where(row == lane, block, 0.0), axis=0, keepdims=True)

    def send_parts(kind):
        half = owners // 2
        left = me < total_devices // 2
        first_count = jnp.where(left, owners - half, half)
        first_base = jnp.where(left, half, 0)
        last_count = owners - first_count
        last_base = half - first_base

        @pl.loop(0, owners)
        def _(turn):
            owner = jnp.where(
                turn < first_count,
                first_base + lax.rem(me + turn, first_count),
                last_base + lax.rem(me + turn, last_count),
            )
            peer = first_owner + owner

            @pl.when(peer != me)
            def _():
                pltpu.make_async_remote_copy(
                    src_ref=part.at[kind, share_rows(owner)],
                    dst_ref=part_in.at[kind, me],
                    send_sem=sum_sems.at[4 * kind],
                    recv_sem=sum_sems.at[4 * kind + 1],
                    device_id=device_of(peer),
                    device_id_type=MESH,
                ).start()

    def share_sum(kind):
        @pl.when(owns)
        def _():
            part_in[kind, me] = part[kind, share_rows(mine), :]
            settle(part_in.at[kind, pl.ds(0, total_devices - 1)], sum_sems.at[4 * kind + 1])
            total = jnp.sum(part_in[kind], axis=0)
            part_own[kind] = total
            whole[kind, share_rows(mine), :] = total

            @pl.loop(0, total_devices - 1)
            def _(turn):
                peer = far_first(me, total_devices, turn)
                pltpu.make_async_remote_copy(
                    src_ref=part_own.at[kind],
                    dst_ref=whole.at[kind, share_rows(mine)],
                    send_sem=sum_sems.at[4 * kind + 2],
                    recv_sem=sum_sems.at[4 * kind + 3],
                    device_id=device_of(peer),
                    device_id_type=MESH,
                ).start()

    def await_sum(kind):
        @pl.when(owns)
        def _():
            settle(whole.at[kind, pl.ds(0, share * (owners - 1))], sum_sems.at[4 * kind + 3])

        @pl.when(jnp.logical_not(owns))
        def _():
            settle(whole.at[kind], sum_sems.at[4 * kind + 3])

    def await_sends(kind):
        @pl.when(owns)
        def _():
            settle(part.at[kind, pl.ds(0, share * (owners - 1))], sum_sems.at[4 * kind])
            settle(part_in.at[kind, pl.ds(0, total_devices - 1)], sum_sems.at[4 * kind + 2])

        @pl.when(jnp.logical_not(owns))
        def _():
            settle(part.at[kind], sum_sems.at[4 * kind])

    part[:, extra_at:, :] = jnp.zeros((2, part.shape[1] - extra_at, 128), jnp.float32)
    stripes = {
        top: jnp.dot(hidden_t[top : top + 128, :], hidden[:, top:], preferred_element_type=jnp.float32)
        for top in range(0, feat, 128)
    }
    for top in tops:
        low = stripes[top + 128][:, :128]
        part[0, pair_at[top] : pair_at[top] + 128, :] = jnp.where(row <= lane, stripes[top][:, :128], low)
        place = extra_at + top // 256
        part[0, place : place + 1, :] = diagonal_row(low)
    for top, side in sides:
        at = side_at[top, side]
        part[0, at : at + 128, :] = stripes[top][:, side - top : side - top + 128]
    send_parts(0)

    for top in tops:
        stripe = jnp.dot(
            features_t[top:, :], hidden[:, top : top + 128], preferred_element_type=jnp.float32
        )
        low = jnp.dot(
            hidden_t[top + 128 : top + 256, :],
            features_ref[...].reshape(rows, feat)[:, top + 128 : top + 256],
            preferred_element_type=jnp.float32,
        )
        part[1, pair_at[top] : pair_at[top] + 128, :] = jnp.where(row >= lane, stripe[:128, :], low)
        place = extra_at + top // 256
        part[1, place : place + 1, :] = diagonal_row(low)
        for side in range(top + 128, feat, 128):
            at = side_at[top, side]
            part[1, at : at + 128, :] = stripe[side - top : side - top + 128, :]
    for top in range(128, feat, 256):
        for side in range(top + 128, feat, 128):
            at = side_at[top, side]
            part[1, at : at + 128, :] = jnp.dot(
                features_t[side : side + 128, :],
                hidden[:, top : top + 128],
                preferred_element_type=jnp.float32,
            )
    square_at = extra_at + feat // 256
    part[1, square_at : square_at + 1, :] = square_row
    send_parts(1)
    share_sum(0)
    share_sum(1)
    await_sum(0)

    vertex_count = rows * total_devices
    diagonal = lax.broadcasted_iota(jnp.int32, (feat, feat), 0) == lax.broadcasted_iota(
        jnp.int32, (feat, feat), 1
    )
    identity = jnp.where(diagonal, 1.0, 0.0)
    inner_identity = epsilon * identity[:128, :128]
    for top in tops:
        pair = whole[0, pair_at[top] : pair_at[top] + 128, :] / vertex_count
        turned = pair.T
        place = extra_at + top // 256
        low_diagonal = whole[0, place : place + 1, :] / vertex_count
        work[top : top + 128, top : top + 128] = jnp.where(row <= lane, pair, turned) + inner_identity
        low = jnp.where(row == lane, low_diagonal, jnp.where(row > lane, pair, turned))
        work[top + 128 : top + 256, top + 128 : top + 256] = low + inner_identity
    for top, side in sides:
        at = side_at[top, side]
        work[top : top + 128, side : side + 128] = whole[0, at : at + 128, :] / vertex_count
        work[side : side + 128, top : top + 128] = jnp.zeros((128, 128), jnp.float32)
    work[:, feat:] = identity
    for start in range(0, feat, LEAF):
        stop = start + LEAF
        inverse = leaf_inverse(work[start:stop, start:stop])
        pivot_rows = jnp.dot(
            inverse, work[start:stop, :], precision=HIGH, preferred_element_type=jnp.float32
        )
        work[start:stop, :] = pivot_rows
        if stop < feat:
            work[stop:, :] = work[stop:, :] - lax.dot_general(
                pivot_rows[:, stop:feat],
                pivot_rows,
                (((0,), (0,)), ((), ())),
                precision=HIGH,
                preferred_element_type=jnp.float32,
            )

    lower_inverse = work[:, feat:]
    high_part = lower_inverse.astype(jnp.bfloat16)
    low_part = (lower_inverse - high_part.astype(jnp.float32)).astype(jnp.bfloat16)
    across = (((1,), (1,)), ((), ()))
    white = lax.dot_general(
        hidden, high_part, across, preferred_element_type=jnp.float32
    ) + lax.dot_general(hidden, low_part, across, preferred_element_type=jnp.float32)
    result[...] = white.astype(jnp.bfloat16)
    store = pltpu.make_async_copy(result, out_ref, load_sems.at[len(loads)])
    store.start()

    settle(far_send.at[pl.ds(0, per_dom * (n_dom - 1))], halo_sems.at[0])
    settle(near_send.at[pl.ds(0, per_sub * (n_sub - 1))], halo_sems.at[2])

    await_sends(0)
    await_sends(1)
    await_sum(1)
    cross = jnp.zeros((128, 128), jnp.float32)
    norm = jnp.zeros((128, 128), jnp.float32)
    for top in tops:
        upper = work[top : top + 128, feat + top : feat + top + 128]
        lower = work[top + 128 : top + 256, feat + top + 128 : feat + top + 256]
        place = extra_at + top // 256
        pair = whole[1, pair_at[top] : pair_at[top] + 128, :]
        low_diagonal = whole[1, place : place + 1, :]
        cross = cross + jnp.where(row >= lane, upper, lower.T) * pair
        cross = cross + jnp.where(row == lane, lower * low_diagonal, 0.0)
        norm = norm + upper * upper + lower * lower
    for top, side in sides:
        at = side_at[top, side]
        across_block = work[side : side + 128, feat + top : feat + top + 128]
        cross = cross + across_block * whole[1, at : at + 128, :]
        norm = norm + across_block * across_block
    rest = jnp.sum(-2.0 * cross - (vertex_count * epsilon) * norm, axis=0, keepdims=True)
    rest = rest + whole[1, square_at : square_at + 1, :]
    loss_ref[0, 0] = 1.0 + jnp.sum(rest) / (vertex_count * feat)
    store.wait()


def body(
    n_dom,
    n_sub,
    features,
    weight,
    send_far,
    send_near,
    tile_dst,
    inner_src,
    outer_src,
    tile_live,
    tile_weight,
):
    rows, feat = features.shape
    size = tile_weight.shape[1]
    slots = inner_src.shape[0]
    total = n_dom * n_sub
    wide = feat // 128
    extra = feat // 256 + 1
    packed_rows = feat // 2 + 64 * wide * (wide - 1) + extra
    share = 8
    while -(-packed_rows // share) > total // 2 + 1:
        share += 8
    packed_rows = -(-packed_rows // share) * share
    far_count = send_far.shape[0]
    near_count = send_near.shape[0]

    def padded(index, peers):
        each = index.shape[0] // peers
        grid = index.reshape(peers, each)
        return jnp.pad(grid, ((0, 0), (0, padded_rows(each) - each))).reshape(1, -1)

    far_index = padded(send_far, n_dom)
    near_index = padded(send_near, n_sub)
    far_padded = far_index.shape[1]
    near_padded = near_index.shape[1]
    anywhere = pl.BlockSpec(memory_space=pl.ANY)
    smem = pl.BlockSpec(memory_space=pltpu.SMEM)
    f32 = jnp.float32
    bf16 = jnp.bfloat16
    whitened, loss = pl.pallas_call(
        functools.partial(kernel, n_dom, n_sub, near_count // n_sub),
        out_shape=(
            jax.ShapeDtypeStruct((rows, feat), bf16),
            jax.ShapeDtypeStruct((1, 1), f32),
        ),
        in_specs=[anywhere] * 9,
        out_specs=(anywhere, smem),
        scratch_shapes=[
            pltpu.VMEM((rows // size, size, feat), bf16),
            pltpu.VMEM(weight.shape, bf16),
            pltpu.VMEM((1, far_padded), jnp.int32),
            pltpu.VMEM((1, near_padded), jnp.int32),
            pltpu.SMEM(tile_dst.shape, jnp.int32),
            pltpu.SMEM(inner_src.shape, jnp.int32),
            pltpu.SMEM(outer_src.shape, jnp.int32),
            pltpu.SMEM(tile_live.shape, jnp.int32),
            pltpu.VMEM(tile_weight.shape, bf16),
            pltpu.VMEM((rows, feat), bf16),
            pltpu.VMEM((far_padded, feat), bf16),
            pltpu.VMEM((near_padded, feat), bf16),
            pltpu.VMEM((far_padded + near_padded, feat), bf16),
            pltpu.VMEM(((far_count + near_count) // size, size, feat), bf16),
            pltpu.VMEM((slots, size, feat), f32),
            pltpu.VMEM((rows // size, size, feat), f32),
            pltpu.VMEM((rows, feat), bf16),
            pltpu.VMEM((feat, rows), bf16),
            pltpu.VMEM((2, packed_rows, 128), f32),
            pltpu.VMEM((2, total, share, 128), f32),
            pltpu.VMEM((2, share, 128), f32),
            pltpu.VMEM((2, packed_rows, 128), f32),
            pltpu.VMEM((feat, 2 * feat), f32),
            pltpu.SemaphoreType.DMA((10,)),
            pltpu.SemaphoreType.DMA((4,)),
            pltpu.SemaphoreType.DMA((8,)),
        ],
        compiler_params=pltpu.CompilerParams(collective_id=0, has_side_effects=True),
    )(
        features.reshape(rows // size, size, feat),
        weight,
        far_index,
        near_index,
        tile_dst,
        inner_src,
        outer_src,
        tile_live,
        tile_weight,
    )
    return whitened, loss.reshape(())


def solution(mesh):
    placed = (
        P(("dom", "sub"), None),
        P(),
        P(("dom", "sub")),
        P(("dom", "sub")),
        P(("dom", "sub")),
        P(("dom", "sub")),
        P(("dom", "sub")),
        P(("dom", "sub"), None),
        P(("dom", "sub"), None, None),
    )
    return jax.shard_map(
        functools.partial(body, mesh.shape["dom"], mesh.shape["sub"]),
        mesh=mesh,
        in_specs=placed,
        out_specs=(P(("dom", "sub"), None), P()),
        check_vma=False,
    )
```

```python
import functools

import jax
import jax.numpy as jnp
from jax import lax
from jax.experimental import pallas as pl
from jax.experimental.pallas import tpu as pltpu
from jax.sharding import PartitionSpec as P

epsilon = 1e-05
MESH = pl.DeviceIdType.MESH
LEAF = 32
GROUP = 16


def one_hot_rows(index_row, row_count):
    rows = index_row.shape[1]
    columns = jnp.broadcast_to(index_row, (128, rows)).T
    lane = lax.broadcasted_iota(jnp.int32, (rows, 128), 1)
    parts = [
        jnp.where(columns == lane + start, 1.0, 0.0).astype(jnp.bfloat16)
        for start in range(0, row_count, 128)
    ]
    return jnp.concatenate(parts, axis=1)


def padded_rows(count):
    return -(-count // 16) * 16


def packing(packed_rows, padded_total, n_dom, n_sub, per_dom, per_sub, near_rows_each):
    near_total = n_sub * near_rows_each
    far_total = packed_rows - near_total
    far_rows_each = far_total // n_dom
    row = lax.broadcasted_iota(jnp.int32, (packed_rows, padded_total), 0)
    column = lax.broadcasted_iota(jnp.int32, (packed_rows, padded_total), 1)
    far_place = row + lax.div(row, far_rows_each) * (per_dom - far_rows_each)
    near_row = row - far_total
    near_place = (
        n_dom * per_dom + near_row + lax.div(near_row, near_rows_each) * (per_sub - near_rows_each)
    )
    place = jnp.where(row < far_total, far_place, near_place)
    return jnp.where(place == column, 1.0, 0.0).astype(jnp.bfloat16)


def thirds(block):
    high = block.astype(jnp.bfloat16)
    rest = block - high.astype(jnp.float32)
    mid = rest.astype(jnp.bfloat16)
    low = (rest - mid.astype(jnp.float32)).astype(jnp.bfloat16)
    return high, mid, low


def factor_rows(lines, lanes):
    count = len(lines[0])
    sub = lax.broadcasted_iota(jnp.int32, (8, 128), 0)
    pivots = [jnp.zeros((8, 128), jnp.float32)] * count
    for start in range(0, 8 * count, GROUP):
        tall = range(start // 8, count)
        columns = []
        for k in range(start, start + GROUP):
            tile, lane = divmod(lanes + k, 128)
            columns.append({
                v: jnp.broadcast_to(lines[tile][v][:, lane : lane + 1], (8, 128)) for v in tall
            })
        for i in range(GROUP):
            home, place = divmod(start + i, 8)
            pivot = jnp.broadcast_to(columns[i][home][place : place + 1, :], (8, 128))
            pivots[home] = jnp.where(sub == place, pivot, pivots[home])
            inverse = 1.0 / pivot
            below = range(home, count)
            factor = {v: columns[i][v] * inverse for v in below}
            for k in range(i + 1, GROUP):
                entry = jnp.broadcast_to(columns[k][home][place : place + 1, :], (8, 128))
                for v in below:
                    columns[k][v] = columns[k][v] - factor[v] * entry
            factor[home] = jnp.where(sub > place, factor[home], 0.0)
            for tile in lines:
                entry = jnp.broadcast_to(tile[home][place : place + 1, :], (8, 128))
                for v in below:
                    tile[v] = tile[v] - factor[v] * entry
    scale = [lax.rsqrt(pivot) for pivot in pivots]
    return [
        jnp.concatenate([line * by for line, by in zip(tile, scale)], axis=0) for tile in lines
    ]


def factor_inverse(work, feat):
    count = LEAF // 8
    for start in range(0, feat, LEAF):
        stop = start + LEAF
        first = start // 128
        tiles = list(range(first, feat // 128 + (stop - 1) // 128 + 1))
        lines = [
            [work[start + 8 * v : start + 8 * v + 8, 128 * t : 128 * t + 128] for v in range(count)]
            for t in tiles
        ]
        done = jnp.concatenate(factor_rows(lines, start - 128 * first), axis=1)
        work[start:stop, 128 * first : 128 * (tiles[-1] + 1)] = done
        if stop < feat:
            high, mid, low = thirds(done)
            left = jnp.concatenate([high, high, mid, high, mid, low], axis=0)
            right = jnp.concatenate([high, mid, high, low, mid, high], axis=0)
            span = slice(128 * (stop // 128), 128 * (tiles[-1] + 1))
            skip = span.start - 128 * first
            for top, bottom in ((stop, stop + LEAF), (stop + LEAF, feat)):
                if top < bottom:
                    update = lax.dot_general(
                        left[:, top - 128 * first : bottom - 128 * first],
                        right[:, skip:],
                        (((0,), (0,)), ((), ())),
                        preferred_element_type=jnp.float32,
                    )
                    work[top:bottom, span] = work[top:bottom, span] - update


def far_first(index, count, turn):
    if count % 2:
        return lax.rem(index + 1 + turn, count)
    half = count // 2
    mine = lax.div(index, half) * half
    other = half - mine
    return jnp.where(
        turn < half,
        other + lax.rem(index + half // 2 + turn, half),
        mine + lax.rem(index + 1 + turn, half),
    )


def kernel(
    n_dom,
    n_sub,
    near_each,
    features_in,
    weight_in,
    far_in,
    near_in,
    dst_in,
    inner_in,
    outer_in,
    live_in,
    tile_in,
    out_ref,
    loss_ref,
    features_ref,
    weight_ref,
    far_ref,
    near_ref,
    dst_ref,
    inner_ref,
    outer_ref,
    live_ref,
    tile_ref,
    result,
    far_send,
    near_send,
    arrived,
    table,
    products,
    acc,
    aggregate,
    features_t,
    part,
    part_in,
    part_own,
    whole,
    work,
    load_sems,
    halo_sems,
    sum_sems,
):
    total_devices = n_dom * n_sub
    dom = lax.axis_index("dom")
    sub = lax.axis_index("sub")
    me = dom * n_sub + sub
    tiles, size, feat = features_ref.shape
    rows = tiles * size
    slots = inner_ref.shape[0]
    share = part_own.shape[1]
    owners = part.shape[1] // share
    first_owner = (total_devices - owners) // 2
    mine = me - first_owner
    owns = jnp.logical_and(mine >= 0, mine < owners)

    def share_rows(owner):
        return pl.ds(pl.multiple_of(owner * share, share), share)

    def device_of(index):
        return (lax.div(index, n_sub), lax.rem(index, n_sub))

    incoming = (
        (far_in, far_ref),
        (near_in, near_ref),
        (features_in, features_ref),
        (inner_in, inner_ref),
        (outer_in, outer_ref),
        (dst_in, dst_ref),
        (live_in, live_ref),
        (tile_in, tile_ref),
        (weight_in, weight_ref),
    )
    loads = [
        pltpu.make_async_copy(source, target, load_sems.at[place])
        for place, (source, target) in enumerate(incoming)
    ]

    barrier = pltpu.get_barrier_semaphore()

    @pl.loop(1, total_devices)
    def _(offset):
        peer = lax.rem(me + offset, total_devices)
        pl.semaphore_signal(barrier, inc=1, device_id=device_of(peer), device_id_type=MESH)

    for load in loads:
        load.start()
    for load in loads[:3]:
        load.wait()

    features = features_ref[...].reshape(rows, feat)
    far_rows = jnp.dot(
        one_hot_rows(far_ref[...], rows), features, preferred_element_type=jnp.float32
    ).astype(jnp.bfloat16)
    near_rows = jnp.dot(
        one_hot_rows(near_ref[...], rows), features, preferred_element_type=jnp.float32
    ).astype(jnp.bfloat16)
    far_send[...] = far_rows
    near_send[...] = near_rows
    per_dom = far_send.shape[0] // n_dom
    per_sub = near_send.shape[0] // n_sub
    far_count = per_dom * n_dom
    packed = size % per_dom == 0 and size % per_sub == 0 and arrived.shape[0] == table.shape[0] * size

    def place(first, count):
        if packed:
            within = pl.multiple_of(lax.rem(first, size), count)
            return table.at[lax.div(first, size), pl.ds(within, count)]
        return arrived.at[pl.ds(pl.multiple_of(first, count), count)]

    def dom_rows(index):
        return pl.ds(pl.multiple_of(index * per_dom, per_dom), per_dom)

    def sub_rows(index):
        return pl.ds(pl.multiple_of(index * per_sub, per_sub), per_sub)

    def dom_place(index):
        return place(index * per_dom, per_dom)

    def sub_place(index):
        return place(far_count + index * per_sub, per_sub)

    pl.semaphore_wait(barrier, total_devices - 1)

    @pl.loop(0, n_dom - 1)
    def _(turn):
        peer = far_first(dom, n_dom, turn)
        pltpu.make_async_remote_copy(
            src_ref=far_send.at[dom_rows(peer)],
            dst_ref=dom_place(dom),
            send_sem=halo_sems.at[0],
            recv_sem=halo_sems.at[1],
            device_id=(peer, sub),
            device_id_type=MESH,
        ).start()

    @pl.loop(0, n_sub - 1)
    def _(turn):
        peer = far_first(sub, n_sub, turn)
        pltpu.make_async_remote_copy(
            src_ref=near_send.at[sub_rows(peer)],
            dst_ref=sub_place(sub),
            send_sem=halo_sems.at[2],
            recv_sem=halo_sems.at[3],
            device_id=(dom, peer),
            device_id_type=MESH,
        ).start()

    dom_place(dom)[...] = far_send[dom_rows(dom), :]
    sub_place(sub)[...] = near_send[sub_rows(sub), :]

    def slot_products(rows_ref, source, first):
        for slot in range(slots):
            products[slot] = jnp.dot(
                tile_ref[first + slot],
                rows_ref[source[slot]],
                preferred_element_type=jnp.float32,
            )

    def slot_sum(tile, first, count):
        total = None
        for slot in range(slots):
            target = jnp.full((1, feat), dst_ref[first + slot], jnp.int32)
            chosen = jnp.where(jnp.logical_and(target == tile, count > slot), 1.0, 0.0)
            term = products[slot] * chosen
            total = term if total is None else total + term
        return total

    for load in loads[3:]:
        load.wait()
    slot_products(features_ref, inner_ref, 0)
    features_t[...] = features.T
    squares = features.astype(jnp.float32)
    squares = jnp.sum(squares * squares, axis=0, keepdims=True)
    square_row = squares[:, :128]
    for side in range(128, feat, 128):
        square_row = square_row + squares[:, side : side + 128]
    inner_count = jnp.full((1, feat), live_ref[0, 0], jnp.int32)
    outer_count = jnp.full((1, feat), live_ref[0, 1], jnp.int32)

    @pl.loop(0, tiles)
    def _(tile):
        acc[tile] = slot_sum(tile, 0, inner_count)

    def settle(ref, sem):
        pltpu.make_async_copy(ref, ref, sem).wait()

    settle(arrived.at[pl.ds(0, per_dom * (n_dom - 1))], halo_sems.at[1])
    settle(arrived.at[pl.ds(0, per_sub * (n_sub - 1))], halo_sems.at[3])
    if not packed:
        table[...] = jnp.dot(
            packing(table.shape[0] * size, arrived.shape[0], n_dom, n_sub, per_dom, per_sub, near_each),
            arrived[...],
            preferred_element_type=jnp.float32,
        ).astype(jnp.bfloat16).reshape(table.shape)
    slot_products(table, outer_ref, slots)

    @pl.loop(0, tiles)
    def _(tile):
        total = acc[tile] + slot_sum(tile, slots, outer_count)
        aggregate[pl.ds(pl.multiple_of(tile * size, size), size), :] = total.astype(jnp.bfloat16)

    projected = jnp.dot(aggregate[...], weight_ref[...], preferred_element_type=jnp.float32)
    hidden = (
        features_ref[...].reshape(rows, feat).astype(jnp.float32) + projected / (1.0 + jnp.exp(-projected))
    ).astype(jnp.bfloat16)
    hidden_t = hidden.T
    row = lax.broadcasted_iota(jnp.int32, (128, 128), 0)
    lane = lax.broadcasted_iota(jnp.int32, (128, 128), 1)
    tops = range(0, feat, 256)
    sides = [(top, side) for top in range(0, feat, 128) for side in range(top + 128, feat, 128)]
    pair_at = {top: top // 2 for top in tops}
    side_at = {pair: feat // 2 + 128 * place for place, pair in enumerate(sides)}
    extra_at = feat // 2 + 128 * len(sides)

    def diagonal_row(block):
        return jnp.sum(jnp.where(row == lane, block, 0.0), axis=0, keepdims=True)

    def send_parts(kind):
        half = owners // 2
        left = me < total_devices // 2
        first_count = jnp.where(left, owners - half, half)
        first_base = jnp.where(left, half, 0)
        last_count = owners - first_count
        last_base = half - first_base

        @pl.loop(0, owners)
        def _(turn):
            owner = jnp.where(
                turn < first_count,
                first_base + lax.rem(me + turn, first_count),
                last_base + lax.rem(me + turn, last_count),
            )
            peer = first_owner + owner

            @pl.when(peer != me)
            def _():
                pltpu.make_async_remote_copy(
                    src_ref=part.at[kind, share_rows(owner)],
                    dst_ref=part_in.at[kind, me],
                    send_sem=sum_sems.at[4 * kind],
                    recv_sem=sum_sems.at[4 * kind + 1],
                    device_id=device_of(peer),
                    device_id_type=MESH,
                ).start()

    def share_sum(kind):
        @pl.when(owns)
        def _():
            part_in[kind, me] = part[kind, share_rows(mine), :]
            settle(part_in.at[kind, pl.ds(0, total_devices - 1)], sum_sems.at[4 * kind + 1])
            total = jnp.sum(part_in[kind], axis=0)
            part_own[kind] = total
            whole[kind, share_rows(mine), :] = total

            @pl.loop(0, total_devices - 1)
            def _(turn):
                peer = far_first(me, total_devices, turn)
                pltpu.make_async_remote_copy(
                    src_ref=part_own.at[kind],
                    dst_ref=whole.at[kind, share_rows(mine)],
                    send_sem=sum_sems.at[4 * kind + 2],
                    recv_sem=sum_sems.at[4 * kind + 3],
                    device_id=device_of(peer),
                    device_id_type=MESH,
                ).start()

    def await_sum(kind):
        @pl.when(owns)
        def _():
            settle(whole.at[kind, pl.ds(0, share * (owners - 1))], sum_sems.at[4 * kind + 3])

        @pl.when(jnp.logical_not(owns))
        def _():
            settle(whole.at[kind], sum_sems.at[4 * kind + 3])

    def await_sends(kind):
        @pl.when(owns)
        def _():
            settle(part.at[kind, pl.ds(0, share * (owners - 1))], sum_sems.at[4 * kind])
            settle(part_in.at[kind, pl.ds(0, total_devices - 1)], sum_sems.at[4 * kind + 2])

        @pl.when(jnp.logical_not(owns))
        def _():
            settle(part.at[kind], sum_sems.at[4 * kind])

    part[:, extra_at:, :] = jnp.zeros((2, part.shape[1] - extra_at, 128), jnp.float32)
    stripes = {
        top: jnp.dot(hidden_t[top : top + 128, :], hidden[:, top:], preferred_element_type=jnp.float32)
        for top in range(0, feat, 128)
    }
    for top in tops:
        low = stripes[top + 128][:, :128]
        part[0, pair_at[top] : pair_at[top] + 128, :] = jnp.where(row <= lane, stripes[top][:, :128], low)
        place = extra_at + top // 256
        part[0, place : place + 1, :] = diagonal_row(low)
    for top, side in sides:
        at = side_at[top, side]
        part[0, at : at + 128, :] = stripes[top][:, side - top : side - top + 128]
    send_parts(0)

    for top in tops:
        stripe = jnp.dot(
            features_t[top:, :], hidden[:, top : top + 128], preferred_element_type=jnp.float32
        )
        low = jnp.dot(
            hidden_t[top + 128 : top + 256, :],
            features_ref[...].reshape(rows, feat)[:, top + 128 : top + 256],
            preferred_element_type=jnp.float32,
        )
        part[1, pair_at[top] : pair_at[top] + 128, :] = jnp.where(row >= lane, stripe[:128, :], low)
        place = extra_at + top // 256
        part[1, place : place + 1, :] = diagonal_row(low)
        for side in range(top + 128, feat, 128):
            at = side_at[top, side]
            part[1, at : at + 128, :] = stripe[side - top : side - top + 128, :]
    for top in range(128, feat, 256):
        for side in range(top + 128, feat, 128):
            at = side_at[top, side]
            part[1, at : at + 128, :] = jnp.dot(
                features_t[side : side + 128, :],
                hidden[:, top : top + 128],
                preferred_element_type=jnp.float32,
            )
    square_at = extra_at + feat // 256
    part[1, square_at : square_at + 1, :] = square_row
    send_parts(1)
    share_sum(0)
    share_sum(1)
    await_sum(0)

    vertex_count = rows * total_devices
    diagonal = lax.broadcasted_iota(jnp.int32, (feat, feat), 0) == lax.broadcasted_iota(
        jnp.int32, (feat, feat), 1
    )
    identity = jnp.where(diagonal, 1.0, 0.0)
    inner_identity = epsilon * identity[:128, :128]
    for top in tops:
        pair = whole[0, pair_at[top] : pair_at[top] + 128, :] / vertex_count
        turned = pair.T
        place = extra_at + top // 256
        low_diagonal = whole[0, place : place + 1, :] / vertex_count
        work[top : top + 128, top : top + 128] = jnp.where(row <= lane, pair, turned) + inner_identity
        low = jnp.where(row == lane, low_diagonal, jnp.where(row > lane, pair, turned))
        work[top + 128 : top + 256, top + 128 : top + 256] = low + inner_identity
    for top, side in sides:
        at = side_at[top, side]
        work[top : top + 128, side : side + 128] = whole[0, at : at + 128, :] / vertex_count
        work[side : side + 128, top : top + 128] = jnp.zeros((128, 128), jnp.float32)
    work[:, feat:] = identity
    factor_inverse(work, feat)

    lower_inverse = work[:, feat:]
    high_part = lower_inverse.astype(jnp.bfloat16)
    low_part = (lower_inverse - high_part.astype(jnp.float32)).astype(jnp.bfloat16)
    across = (((1,), (1,)), ((), ()))
    white = lax.dot_general(
        hidden, high_part, across, preferred_element_type=jnp.float32
    ) + lax.dot_general(hidden, low_part, across, preferred_element_type=jnp.float32)
    result[...] = white.astype(jnp.bfloat16)
    store = pltpu.make_async_copy(result, out_ref, load_sems.at[len(loads)])
    store.start()

    settle(far_send.at[pl.ds(0, per_dom * (n_dom - 1))], halo_sems.at[0])
    settle(near_send.at[pl.ds(0, per_sub * (n_sub - 1))], halo_sems.at[2])

    await_sends(0)
    await_sends(1)
    await_sum(1)
    cross = jnp.zeros((128, 128), jnp.float32)
    norm = jnp.zeros((128, 128), jnp.float32)
    for top in tops:
        upper = work[top : top + 128, feat + top : feat + top + 128]
        lower = work[top + 128 : top + 256, feat + top + 128 : feat + top + 256]
        place = extra_at + top // 256
        pair = whole[1, pair_at[top] : pair_at[top] + 128, :]
        low_diagonal = whole[1, place : place + 1, :]
        cross = cross + jnp.where(row >= lane, upper, lower.T) * pair
        cross = cross + jnp.where(row == lane, lower * low_diagonal, 0.0)
        norm = norm + upper * upper + lower * lower
    for top, side in sides:
        at = side_at[top, side]
        across_block = work[side : side + 128, feat + top : feat + top + 128]
        cross = cross + across_block * whole[1, at : at + 128, :]
        norm = norm + across_block * across_block
    rest = jnp.sum(-2.0 * cross - (vertex_count * epsilon) * norm, axis=0, keepdims=True)
    rest = rest + whole[1, square_at : square_at + 1, :]
    loss_ref[0, 0] = 1.0 + jnp.sum(rest) / (vertex_count * feat)
    store.wait()


def body(
    n_dom,
    n_sub,
    features,
    weight,
    send_far,
    send_near,
    tile_dst,
    inner_src,
    outer_src,
    tile_live,
    tile_weight,
):
    rows, feat = features.shape
    size = tile_weight.shape[1]
    slots = inner_src.shape[0]
    total = n_dom * n_sub
    wide = feat // 128
    extra = feat // 256 + 1
    packed_rows = feat // 2 + 64 * wide * (wide - 1) + extra
    share = 8
    while -(-packed_rows // share) > total // 2 + 1:
        share += 8
    packed_rows = -(-packed_rows // share) * share
    far_count = send_far.shape[0]
    near_count = send_near.shape[0]

    def padded(index, peers):
        each = index.shape[0] // peers
        grid = index.reshape(peers, each)
        return jnp.pad(grid, ((0, 0), (0, padded_rows(each) - each))).reshape(1, -1)

    far_index = padded(send_far, n_dom)
    near_index = padded(send_near, n_sub)
    far_padded = far_index.shape[1]
    near_padded = near_index.shape[1]
    anywhere = pl.BlockSpec(memory_space=pl.ANY)
    smem = pl.BlockSpec(memory_space=pltpu.SMEM)
    f32 = jnp.float32
    bf16 = jnp.bfloat16
    whitened, loss = pl.pallas_call(
        functools.partial(kernel, n_dom, n_sub, near_count // n_sub),
        out_shape=(
            jax.ShapeDtypeStruct((rows, feat), bf16),
            jax.ShapeDtypeStruct((1, 1), f32),
        ),
        in_specs=[anywhere] * 9,
        out_specs=(anywhere, smem),
        scratch_shapes=[
            pltpu.VMEM((rows // size, size, feat), bf16),
            pltpu.VMEM(weight.shape, bf16),
            pltpu.VMEM((1, far_padded), jnp.int32),
            pltpu.VMEM((1, near_padded), jnp.int32),
            pltpu.SMEM(tile_dst.shape, jnp.int32),
            pltpu.SMEM(inner_src.shape, jnp.int32),
            pltpu.SMEM(outer_src.shape, jnp.int32),
            pltpu.SMEM(tile_live.shape, jnp.int32),
            pltpu.VMEM(tile_weight.shape, bf16),
            pltpu.VMEM((rows, feat), bf16),
            pltpu.VMEM((far_padded, feat), bf16),
            pltpu.VMEM((near_padded, feat), bf16),
            pltpu.VMEM((far_padded + near_padded, feat), bf16),
            pltpu.VMEM(((far_count + near_count) // size, size, feat), bf16),
            pltpu.VMEM((slots, size, feat), f32),
            pltpu.VMEM((rows // size, size, feat), f32),
            pltpu.VMEM((rows, feat), bf16),
            pltpu.VMEM((feat, rows), bf16),
            pltpu.VMEM((2, packed_rows, 128), f32),
            pltpu.VMEM((2, total, share, 128), f32),
            pltpu.VMEM((2, share, 128), f32),
            pltpu.VMEM((2, packed_rows, 128), f32),
            pltpu.VMEM((feat, 2 * feat), f32),
            pltpu.SemaphoreType.DMA((10,)),
            pltpu.SemaphoreType.DMA((4,)),
            pltpu.SemaphoreType.DMA((8,)),
        ],
        compiler_params=pltpu.CompilerParams(collective_id=0, has_side_effects=True),
    )(
        features.reshape(rows // size, size, feat),
        weight,
        far_index,
        near_index,
        tile_dst,
        inner_src,
        outer_src,
        tile_live,
        tile_weight,
    )
    return whitened, loss.reshape(())


def solution(mesh):
    placed = (
        P(("dom", "sub"), None),
        P(),
        P(("dom", "sub")),
        P(("dom", "sub")),
        P(("dom", "sub")),
        P(("dom", "sub")),
        P(("dom", "sub")),
        P(("dom", "sub"), None),
        P(("dom", "sub"), None, None),
    )
    return jax.shard_map(
        functools.partial(body, mesh.shape["dom"], mesh.shape["sub"]),
        mesh=mesh,
        in_specs=placed,
        out_specs=(P(("dom", "sub"), None), P()),
        check_vma=False,
    )
```

```python
import functools

import jax
import jax.numpy as jnp
from jax import lax
from jax.experimental import pallas as pl
from jax.experimental.pallas import tpu as pltpu
from jax.sharding import PartitionSpec as P

epsilon = 1e-05
MESH = pl.DeviceIdType.MESH
LEAF = 32
GROUP = 16
CHUNKS = 4
VMEM_LIMIT = 32 * 1024 * 1024


def one_hot_rows(index_row, row_count):
    rows = index_row.shape[1]
    columns = jnp.broadcast_to(index_row, (128, rows)).T
    lane = lax.broadcasted_iota(jnp.int32, (rows, 128), 1)
    parts = [
        jnp.where(columns == lane + start, 1.0, 0.0).astype(jnp.bfloat16)
        for start in range(0, row_count, 128)
    ]
    return jnp.concatenate(parts, axis=1)


def padded_rows(count):
    return -(-count // 16) * 16


def packing(packed_rows, padded_total, n_dom, n_sub, per_dom, per_sub, near_rows_each):
    near_total = n_sub * near_rows_each
    far_total = packed_rows - near_total
    far_rows_each = far_total // n_dom
    row = lax.broadcasted_iota(jnp.int32, (packed_rows, padded_total), 0)
    column = lax.broadcasted_iota(jnp.int32, (packed_rows, padded_total), 1)
    far_place = row + lax.div(row, far_rows_each) * (per_dom - far_rows_each)
    near_row = row - far_total
    near_place = (
        n_dom * per_dom + near_row + lax.div(near_row, near_rows_each) * (per_sub - near_rows_each)
    )
    place = jnp.where(row < far_total, far_place, near_place)
    return jnp.where(place == column, 1.0, 0.0).astype(jnp.bfloat16)


def thirds(block):
    high = block.astype(jnp.bfloat16)
    rest = block - high.astype(jnp.float32)
    mid = rest.astype(jnp.bfloat16)
    low = (rest - mid.astype(jnp.float32)).astype(jnp.bfloat16)
    return high, mid, low


def factor_rows(lines, lanes):
    count = len(lines[0])
    sub = lax.broadcasted_iota(jnp.int32, (8, 128), 0)
    pivots = [jnp.zeros((8, 128), jnp.float32)] * count
    for start in range(0, 8 * count, GROUP):
        tall = range(start // 8, count)
        columns = []
        for k in range(start, start + GROUP):
            tile, lane = divmod(lanes + k, 128)
            columns.append({
                v: jnp.broadcast_to(lines[tile][v][:, lane : lane + 1], (8, 128)) for v in tall
            })
        for i in range(GROUP):
            home, place = divmod(start + i, 8)
            pivot = jnp.broadcast_to(columns[i][home][place : place + 1, :], (8, 128))
            pivots[home] = jnp.where(sub == place, pivot, pivots[home])
            inverse = 1.0 / pivot
            below = range(home, count)
            factor = {v: columns[i][v] * inverse for v in below}
            for k in range(i + 1, GROUP):
                entry = jnp.broadcast_to(columns[k][home][place : place + 1, :], (8, 128))
                for v in below:
                    columns[k][v] = columns[k][v] - factor[v] * entry
            factor[home] = jnp.where(sub > place, factor[home], 0.0)
            for tile in lines:
                entry = jnp.broadcast_to(tile[home][place : place + 1, :], (8, 128))
                for v in below:
                    tile[v] = tile[v] - factor[v] * entry
    scale = [lax.rsqrt(pivot) for pivot in pivots]
    return [
        jnp.concatenate([line * by for line, by in zip(tile, scale)], axis=0) for tile in lines
    ]


def factor_inverse(work, feat):
    count = LEAF // 8
    for start in range(0, feat, LEAF):
        stop = start + LEAF
        first = start // 128
        tiles = list(range(first, feat // 128 + (stop - 1) // 128 + 1))
        lines = [
            [work[start + 8 * v : start + 8 * v + 8, 128 * t : 128 * t + 128] for v in range(count)]
            for t in tiles
        ]
        done = jnp.concatenate(factor_rows(lines, start - 128 * first), axis=1)
        work[start:stop, 128 * first : 128 * (tiles[-1] + 1)] = done
        if stop < feat:
            high, mid, low = thirds(done)
            left = jnp.concatenate([high, high, mid, high, mid, low], axis=0)
            right = jnp.concatenate([high, mid, high, low, mid, high], axis=0)
            span = slice(128 * (stop // 128), 128 * (tiles[-1] + 1))
            skip = span.start - 128 * first
            for top, bottom in ((stop, stop + LEAF), (stop + LEAF, feat)):
                if top < bottom:
                    update = lax.dot_general(
                        left[:, top - 128 * first : bottom - 128 * first],
                        right[:, skip:],
                        (((0,), (0,)), ((), ())),
                        preferred_element_type=jnp.float32,
                    )
                    work[top:bottom, span] = work[top:bottom, span] - update


def far_first(index, count, turn):
    if count % 2:
        return lax.rem(index + 1 + turn, count)
    half = count // 2
    mine = lax.div(index, half) * half
    other = half - mine
    return jnp.where(
        turn < half,
        other + lax.rem(index + half // 2 + turn, half),
        mine + lax.rem(index + 1 + turn, half),
    )


def kernel(
    n_dom,
    n_sub,
    near_each,
    features_in,
    weight_in,
    far_in,
    near_in,
    dst_in,
    inner_in,
    outer_in,
    live_in,
    tile_in,
    hidden_ref,
    inverse_ref,
    loss_ref,
    features_ref,
    weight_ref,
    far_ref,
    near_ref,
    dst_ref,
    inner_ref,
    outer_ref,
    live_ref,
    tile_ref,
    far_send,
    near_send,
    arrived,
    table,
    products,
    acc,
    aggregate,
    features_t,
    part,
    part_in,
    part_own,
    whole,
    work,
    load_sems,
    halo_sems,
    sum_sems,
):
    total_devices = n_dom * n_sub
    dom = lax.axis_index("dom")
    sub = lax.axis_index("sub")
    me = dom * n_sub + sub
    tiles, size, feat = features_ref.shape
    rows = tiles * size
    slots = inner_ref.shape[0]
    share = part_own.shape[1]
    owners = part.shape[1] // share
    first_owner = (total_devices - owners) // 2
    mine = me - first_owner
    owns = jnp.logical_and(mine >= 0, mine < owners)

    def share_rows(owner):
        return pl.ds(pl.multiple_of(owner * share, share), share)

    def device_of(index):
        return (lax.div(index, n_sub), lax.rem(index, n_sub))

    incoming = (
        (far_in, far_ref),
        (near_in, near_ref),
        (features_in, features_ref),
        (inner_in, inner_ref),
        (outer_in, outer_ref),
        (dst_in, dst_ref),
        (live_in, live_ref),
        (tile_in, tile_ref),
        (weight_in, weight_ref),
    )
    loads = [
        pltpu.make_async_copy(source, target, load_sems.at[place])
        for place, (source, target) in enumerate(incoming)
    ]

    barrier = pltpu.get_barrier_semaphore()

    @pl.loop(1, total_devices)
    def _(offset):
        peer = lax.rem(me + offset, total_devices)
        pl.semaphore_signal(barrier, inc=1, device_id=device_of(peer), device_id_type=MESH)

    for load in loads:
        load.start()
    for load in loads[:3]:
        load.wait()

    features = features_ref[...].reshape(rows, feat)
    far_rows = jnp.dot(
        one_hot_rows(far_ref[...], rows), features, preferred_element_type=jnp.float32
    ).astype(jnp.bfloat16)
    near_rows = jnp.dot(
        one_hot_rows(near_ref[...], rows), features, preferred_element_type=jnp.float32
    ).astype(jnp.bfloat16)
    far_send[...] = far_rows
    near_send[...] = near_rows
    per_dom = far_send.shape[0] // n_dom
    per_sub = near_send.shape[0] // n_sub
    far_count = per_dom * n_dom
    packed = size % per_dom == 0 and size % per_sub == 0 and arrived.shape[0] == table.shape[0] * size

    def place(first, count):
        if packed:
            within = pl.multiple_of(lax.rem(first, size), count)
            return table.at[lax.div(first, size), pl.ds(within, count)]
        return arrived.at[pl.ds(pl.multiple_of(first, count), count)]

    def dom_rows(index):
        return pl.ds(pl.multiple_of(index * per_dom, per_dom), per_dom)

    def sub_rows(index):
        return pl.ds(pl.multiple_of(index * per_sub, per_sub), per_sub)

    def dom_place(index):
        return place(index * per_dom, per_dom)

    def sub_place(index):
        return place(far_count + index * per_sub, per_sub)

    pl.semaphore_wait(barrier, total_devices - 1)

    @pl.loop(0, n_dom - 1)
    def _(turn):
        peer = far_first(dom, n_dom, turn)
        pltpu.make_async_remote_copy(
            src_ref=far_send.at[dom_rows(peer)],
            dst_ref=dom_place(dom),
            send_sem=halo_sems.at[0],
            recv_sem=halo_sems.at[1],
            device_id=(peer, sub),
            device_id_type=MESH,
        ).start()

    @pl.loop(0, n_sub - 1)
    def _(turn):
        peer = far_first(sub, n_sub, turn)
        pltpu.make_async_remote_copy(
            src_ref=near_send.at[sub_rows(peer)],
            dst_ref=sub_place(sub),
            send_sem=halo_sems.at[2],
            recv_sem=halo_sems.at[3],
            device_id=(dom, peer),
            device_id_type=MESH,
        ).start()

    dom_place(dom)[...] = far_send[dom_rows(dom), :]
    sub_place(sub)[...] = near_send[sub_rows(sub), :]

    def slot_products(rows_ref, source, first):
        for slot in range(slots):
            products[slot] = jnp.dot(
                tile_ref[first + slot],
                rows_ref[source[slot]],
                preferred_element_type=jnp.float32,
            )

    def slot_sum(tile, first, count):
        total = None
        for slot in range(slots):
            target = jnp.full((1, feat), dst_ref[first + slot], jnp.int32)
            chosen = jnp.where(jnp.logical_and(target == tile, count > slot), 1.0, 0.0)
            term = products[slot] * chosen
            total = term if total is None else total + term
        return total

    for load in loads[3:]:
        load.wait()
    slot_products(features_ref, inner_ref, 0)
    features_t[...] = features.T
    squares = features.astype(jnp.float32)
    squares = jnp.sum(squares * squares, axis=0, keepdims=True)
    square_row = squares[:, :128]
    for side in range(128, feat, 128):
        square_row = square_row + squares[:, side : side + 128]
    inner_count = jnp.full((1, feat), live_ref[0, 0], jnp.int32)
    outer_count = jnp.full((1, feat), live_ref[0, 1], jnp.int32)

    @pl.loop(0, tiles)
    def _(tile):
        acc[tile] = slot_sum(tile, 0, inner_count)

    def settle(ref, sem):
        pltpu.make_async_copy(ref, ref, sem).wait()

    settle(arrived.at[pl.ds(0, per_dom * (n_dom - 1))], halo_sems.at[1])
    settle(arrived.at[pl.ds(0, per_sub * (n_sub - 1))], halo_sems.at[3])
    if not packed:
        table[...] = jnp.dot(
            packing(table.shape[0] * size, arrived.shape[0], n_dom, n_sub, per_dom, per_sub, near_each),
            arrived[...],
            preferred_element_type=jnp.float32,
        ).astype(jnp.bfloat16).reshape(table.shape)
    slot_products(table, outer_ref, slots)

    @pl.loop(0, tiles)
    def _(tile):
        total = acc[tile] + slot_sum(tile, slots, outer_count)
        aggregate[pl.ds(pl.multiple_of(tile * size, size), size), :] = total.astype(jnp.bfloat16)

    projected = jnp.dot(aggregate[...], weight_ref[...], preferred_element_type=jnp.float32)
    hidden = (
        features_ref[...].reshape(rows, feat).astype(jnp.float32) + projected / (1.0 + jnp.exp(-projected))
    ).astype(jnp.bfloat16)
    hidden_ref[...] = hidden
    hidden_t = hidden.T
    row = lax.broadcasted_iota(jnp.int32, (128, 128), 0)
    lane = lax.broadcasted_iota(jnp.int32, (128, 128), 1)
    tops = range(0, feat, 256)
    sides = [(top, side) for top in range(0, feat, 128) for side in range(top + 128, feat, 128)]
    pair_at = {top: top // 2 for top in tops}
    side_at = {pair: feat // 2 + 128 * place for place, pair in enumerate(sides)}
    extra_at = feat // 2 + 128 * len(sides)

    def diagonal_row(block):
        return jnp.sum(jnp.where(row == lane, block, 0.0), axis=0, keepdims=True)

    def send_parts(kind):
        half = owners // 2
        left = me < total_devices // 2
        first_count = jnp.where(left, owners - half, half)
        first_base = jnp.where(left, half, 0)
        last_count = owners - first_count
        last_base = half - first_base

        @pl.loop(0, owners)
        def _(turn):
            owner = jnp.where(
                turn < first_count,
                first_base + lax.rem(me + turn, first_count),
                last_base + lax.rem(me + turn, last_count),
            )
            peer = first_owner + owner

            @pl.when(peer != me)
            def _():
                pltpu.make_async_remote_copy(
                    src_ref=part.at[kind, share_rows(owner)],
                    dst_ref=part_in.at[kind, me],
                    send_sem=sum_sems.at[4 * kind],
                    recv_sem=sum_sems.at[4 * kind + 1],
                    device_id=device_of(peer),
                    device_id_type=MESH,
                ).start()

    def share_sum(kind):
        @pl.when(owns)
        def _():
            part_in[kind, me] = part[kind, share_rows(mine), :]
            settle(part_in.at[kind, pl.ds(0, total_devices - 1)], sum_sems.at[4 * kind + 1])
            total = jnp.sum(part_in[kind], axis=0)
            part_own[kind] = total
            whole[kind, share_rows(mine), :] = total

            @pl.loop(0, total_devices - 1)
            def _(turn):
                peer = far_first(me, total_devices, turn)
                pltpu.make_async_remote_copy(
                    src_ref=part_own.at[kind],
                    dst_ref=whole.at[kind, share_rows(mine)],
                    send_sem=sum_sems.at[4 * kind + 2],
                    recv_sem=sum_sems.at[4 * kind + 3],
                    device_id=device_of(peer),
                    device_id_type=MESH,
                ).start()

    def await_sum(kind):
        @pl.when(owns)
        def _():
            settle(whole.at[kind, pl.ds(0, share * (owners - 1))], sum_sems.at[4 * kind + 3])

        @pl.when(jnp.logical_not(owns))
        def _():
            settle(whole.at[kind], sum_sems.at[4 * kind + 3])

    def await_sends(kind):
        @pl.when(owns)
        def _():
            settle(part.at[kind, pl.ds(0, share * (owners - 1))], sum_sems.at[4 * kind])
            settle(part_in.at[kind, pl.ds(0, total_devices - 1)], sum_sems.at[4 * kind + 2])

        @pl.when(jnp.logical_not(owns))
        def _():
            settle(part.at[kind], sum_sems.at[4 * kind])

    part[:, extra_at:, :] = jnp.zeros((2, part.shape[1] - extra_at, 128), jnp.float32)
    stripes = {
        top: jnp.dot(hidden_t[top : top + 128, :], hidden[:, top:], preferred_element_type=jnp.float32)
        for top in range(0, feat, 128)
    }
    for top in tops:
        low = stripes[top + 128][:, :128]
        part[0, pair_at[top] : pair_at[top] + 128, :] = jnp.where(row <= lane, stripes[top][:, :128], low)
        place = extra_at + top // 256
        part[0, place : place + 1, :] = diagonal_row(low)
    for top, side in sides:
        at = side_at[top, side]
        part[0, at : at + 128, :] = stripes[top][:, side - top : side - top + 128]
    send_parts(0)

    for top in tops:
        stripe = jnp.dot(
            features_t[top:, :], hidden[:, top : top + 128], preferred_element_type=jnp.float32
        )
        low = jnp.dot(
            hidden_t[top + 128 : top + 256, :],
            features_ref[...].reshape(rows, feat)[:, top + 128 : top + 256],
            preferred_element_type=jnp.float32,
        )
        part[1, pair_at[top] : pair_at[top] + 128, :] = jnp.where(row >= lane, stripe[:128, :], low)
        place = extra_at + top // 256
        part[1, place : place + 1, :] = diagonal_row(low)
        for side in range(top + 128, feat, 128):
            at = side_at[top, side]
            part[1, at : at + 128, :] = stripe[side - top : side - top + 128, :]
    for top in range(128, feat, 256):
        for side in range(top + 128, feat, 128):
            at = side_at[top, side]
            part[1, at : at + 128, :] = jnp.dot(
                features_t[side : side + 128, :],
                hidden[:, top : top + 128],
                preferred_element_type=jnp.float32,
            )
    square_at = extra_at + feat // 256
    part[1, square_at : square_at + 1, :] = square_row
    send_parts(1)
    share_sum(0)
    share_sum(1)
    await_sum(0)

    vertex_count = rows * total_devices
    diagonal = lax.broadcasted_iota(jnp.int32, (feat, feat), 0) == lax.broadcasted_iota(
        jnp.int32, (feat, feat), 1
    )
    identity = jnp.where(diagonal, 1.0, 0.0)
    inner_identity = epsilon * identity[:128, :128]
    for top in tops:
        pair = whole[0, pair_at[top] : pair_at[top] + 128, :] / vertex_count
        turned = pair.T
        place = extra_at + top // 256
        low_diagonal = whole[0, place : place + 1, :] / vertex_count
        work[top : top + 128, top : top + 128] = jnp.where(row <= lane, pair, turned) + inner_identity
        low = jnp.where(row == lane, low_diagonal, jnp.where(row > lane, pair, turned))
        work[top + 128 : top + 256, top + 128 : top + 256] = low + inner_identity
    for top, side in sides:
        at = side_at[top, side]
        work[top : top + 128, side : side + 128] = whole[0, at : at + 128, :] / vertex_count
        work[side : side + 128, top : top + 128] = jnp.zeros((128, 128), jnp.float32)
    work[:, feat:] = identity
    factor_inverse(work, feat)

    lower_inverse = work[:, feat:]
    high_part = lower_inverse.astype(jnp.bfloat16)
    low_part = (lower_inverse - high_part.astype(jnp.float32)).astype(jnp.bfloat16)
    inverse_ref[0] = high_part
    inverse_ref[1] = low_part

    settle(far_send.at[pl.ds(0, per_dom * (n_dom - 1))], halo_sems.at[0])
    settle(near_send.at[pl.ds(0, per_sub * (n_sub - 1))], halo_sems.at[2])

    await_sends(0)
    await_sends(1)
    await_sum(1)
    cross = jnp.zeros((128, 128), jnp.float32)
    norm = jnp.zeros((128, 128), jnp.float32)
    for top in tops:
        upper = work[top : top + 128, feat + top : feat + top + 128]
        lower = work[top + 128 : top + 256, feat + top + 128 : feat + top + 256]
        place = extra_at + top // 256
        pair = whole[1, pair_at[top] : pair_at[top] + 128, :]
        low_diagonal = whole[1, place : place + 1, :]
        cross = cross + jnp.where(row >= lane, upper, lower.T) * pair
        cross = cross + jnp.where(row == lane, lower * low_diagonal, 0.0)
        norm = norm + upper * upper + lower * lower
    for top, side in sides:
        at = side_at[top, side]
        across_block = work[side : side + 128, feat + top : feat + top + 128]
        cross = cross + across_block * whole[1, at : at + 128, :]
        norm = norm + across_block * across_block
    rest = jnp.sum(-2.0 * cross - (vertex_count * epsilon) * norm, axis=0, keepdims=True)
    rest = rest + whole[1, square_at : square_at + 1, :]
    loss_ref[0, 0] = 1.0 + jnp.sum(rest) / (vertex_count * feat)


def whiten(hidden_ref, inverse_ref, loss_in, out_ref, loss_ref, result, sems):
    rows = hidden_ref.shape[0]
    across = (((1,), (1,)), ((), ()))
    step = rows // CHUNKS
    stores = []
    for chunk in range(CHUNKS):
        here = pl.ds(chunk * step, step)
        hidden = hidden_ref[here, :]
        white = lax.dot_general(
            hidden, inverse_ref[0], across, preferred_element_type=jnp.float32
        ) + lax.dot_general(hidden, inverse_ref[1], across, preferred_element_type=jnp.float32)
        result[here, :] = white.astype(jnp.bfloat16)
        store = pltpu.make_async_copy(result.at[here], out_ref.at[here], sems.at[chunk])
        store.start()
        stores.append(store)
    loss_ref[0, 0] = loss_in[0, 0]
    for store in stores:
        store.wait()


def body(
    n_dom,
    n_sub,
    features,
    weight,
    send_far,
    send_near,
    tile_dst,
    inner_src,
    outer_src,
    tile_live,
    tile_weight,
):
    rows, feat = features.shape
    size = tile_weight.shape[1]
    slots = inner_src.shape[0]
    total = n_dom * n_sub
    wide = feat // 128
    extra = feat // 256 + 1
    packed_rows = feat // 2 + 64 * wide * (wide - 1) + extra
    share = 8
    while -(-packed_rows // share) > total // 2 + 1:
        share += 8
    packed_rows = -(-packed_rows // share) * share
    far_count = send_far.shape[0]
    near_count = send_near.shape[0]

    def padded(index, peers):
        each = index.shape[0] // peers
        grid = index.reshape(peers, each)
        return jnp.pad(grid, ((0, 0), (0, padded_rows(each) - each))).reshape(1, -1)

    far_index = padded(send_far, n_dom)
    near_index = padded(send_near, n_sub)
    far_padded = far_index.shape[1]
    near_padded = near_index.shape[1]
    anywhere = pl.BlockSpec(memory_space=pltpu.HBM)
    smem = pl.BlockSpec(memory_space=pltpu.SMEM)
    f32 = jnp.float32
    bf16 = jnp.bfloat16
    vmem = pl.BlockSpec(memory_space=pltpu.VMEM)
    hidden, inverse, loss = pl.pallas_call(
        functools.partial(kernel, n_dom, n_sub, near_count // n_sub),
        out_shape=(
            pltpu.VMEM((rows, feat), bf16),
            pltpu.VMEM((2, feat, feat), bf16),
            jax.ShapeDtypeStruct((1, 1), f32),
        ),
        in_specs=[anywhere] * 9,
        out_specs=(vmem, vmem, smem),
        scratch_shapes=[
            pltpu.VMEM((rows // size, size, feat), bf16),
            pltpu.VMEM(weight.shape, bf16),
            pltpu.VMEM((1, far_padded), jnp.int32),
            pltpu.VMEM((1, near_padded), jnp.int32),
            pltpu.SMEM(tile_dst.shape, jnp.int32),
            pltpu.SMEM(inner_src.shape, jnp.int32),
            pltpu.SMEM(outer_src.shape, jnp.int32),
            pltpu.SMEM(tile_live.shape, jnp.int32),
            pltpu.VMEM(tile_weight.shape, bf16),
            pltpu.VMEM((far_padded, feat), bf16),
            pltpu.VMEM((near_padded, feat), bf16),
            pltpu.VMEM((far_padded + near_padded, feat), bf16),
            pltpu.VMEM(((far_count + near_count) // size, size, feat), bf16),
            pltpu.VMEM((slots, size, feat), f32),
            pltpu.VMEM((rows // size, size, feat), f32),
            pltpu.VMEM((rows, feat), bf16),
            pltpu.VMEM((feat, rows), bf16),
            pltpu.VMEM((2, packed_rows, 128), f32),
            pltpu.VMEM((2, total, share, 128), f32),
            pltpu.VMEM((2, share, 128), f32),
            pltpu.VMEM((2, packed_rows, 128), f32),
            pltpu.VMEM((feat, 2 * feat), f32),
            pltpu.SemaphoreType.DMA((10,)),
            pltpu.SemaphoreType.DMA((4,)),
            pltpu.SemaphoreType.DMA((8,)),
        ],
        compiler_params=pltpu.CompilerParams(
            collective_id=0, has_side_effects=True, vmem_limit_bytes=VMEM_LIMIT
        ),
    )(
        *[
            pltpu.with_memory_space_constraint(value, pltpu.HBM)
            for value in (
                features.reshape(rows // size, size, feat),
                weight,
                far_index,
                near_index,
                tile_dst,
                inner_src,
                outer_src,
                tile_live,
                tile_weight,
            )
        ]
    )
    whitened, loss = pl.pallas_call(
        whiten,
        out_shape=(
            jax.ShapeDtypeStruct((rows, feat), bf16),
            jax.ShapeDtypeStruct((1, 1), f32),
        ),
        in_specs=[vmem, vmem, smem],
        out_specs=(anywhere, smem),
        scratch_shapes=[pltpu.VMEM((rows, feat), bf16), pltpu.SemaphoreType.DMA((CHUNKS,))],
        compiler_params=pltpu.CompilerParams(vmem_limit_bytes=VMEM_LIMIT),
    )(hidden, inverse, loss)
    return whitened, loss.reshape(())


def solution(mesh):
    placed = (
        P(("dom", "sub"), None),
        P(),
        P(("dom", "sub")),
        P(("dom", "sub")),
        P(("dom", "sub")),
        P(("dom", "sub")),
        P(("dom", "sub")),
        P(("dom", "sub"), None),
        P(("dom", "sub"), None, None),
    )
    return jax.shard_map(
        functools.partial(body, mesh.shape["dom"], mesh.shape["sub"]),
        mesh=mesh,
        in_specs=placed,
        out_specs=(P(("dom", "sub"), None), P()),
        check_vma=False,
    )
```

```python
import functools

import jax
import jax.numpy as jnp
from jax import lax
from jax.experimental import pallas as pl
from jax.experimental.pallas import tpu as pltpu
from jax.sharding import PartitionSpec as P

epsilon = 1e-05
MESH = pl.DeviceIdType.MESH
LEAF = 32
GROUP = 16
CHUNKS = 4
VMEM_LIMIT = 32 * 1024 * 1024


def one_hot_rows(index_row, row_count):
    rows = index_row.shape[1]
    columns = jnp.broadcast_to(index_row, (128, rows)).T
    lane = lax.broadcasted_iota(jnp.int32, (rows, 128), 1)
    parts = [
        jnp.where(columns == lane + start, 1.0, 0.0).astype(jnp.bfloat16)
        for start in range(0, row_count, 128)
    ]
    return jnp.concatenate(parts, axis=1)


def padded_rows(count):
    return -(-count // 16) * 16


def packing(packed_rows, padded_total, n_dom, n_sub, per_dom, per_sub, near_rows_each):
    near_total = n_sub * near_rows_each
    far_total = packed_rows - near_total
    far_rows_each = far_total // n_dom
    row = lax.broadcasted_iota(jnp.int32, (packed_rows, padded_total), 0)
    column = lax.broadcasted_iota(jnp.int32, (packed_rows, padded_total), 1)
    far_place = row + lax.div(row, far_rows_each) * (per_dom - far_rows_each)
    near_row = row - far_total
    near_place = (
        n_dom * per_dom + near_row + lax.div(near_row, near_rows_each) * (per_sub - near_rows_each)
    )
    place = jnp.where(row < far_total, far_place, near_place)
    return jnp.where(place == column, 1.0, 0.0).astype(jnp.bfloat16)


def thirds(block):
    high = block.astype(jnp.bfloat16)
    rest = block - high.astype(jnp.float32)
    mid = rest.astype(jnp.bfloat16)
    low = (rest - mid.astype(jnp.float32)).astype(jnp.bfloat16)
    return high, mid, low


def factor_rows(lines, lanes):
    count = len(lines[0])
    sub = lax.broadcasted_iota(jnp.int32, (8, 128), 0)
    pivots = [jnp.zeros((8, 128), jnp.float32)] * count
    for start in range(0, 8 * count, GROUP):
        tall = range(start // 8, count)
        columns = []
        for k in range(start, start + GROUP):
            tile, lane = divmod(lanes + k, 128)
            columns.append({
                v: jnp.broadcast_to(lines[tile][v][:, lane : lane + 1], (8, 128)) for v in tall
            })
        for i in range(GROUP):
            home, place = divmod(start + i, 8)
            pivot = jnp.broadcast_to(columns[i][home][place : place + 1, :], (8, 128))
            pivots[home] = jnp.where(sub == place, pivot, pivots[home])
            inverse = 1.0 / pivot
            below = range(home, count)
            factor = {v: columns[i][v] * inverse for v in below}
            for k in range(i + 1, GROUP):
                entry = jnp.broadcast_to(columns[k][home][place : place + 1, :], (8, 128))
                for v in below:
                    columns[k][v] = columns[k][v] - factor[v] * entry
            factor[home] = jnp.where(sub > place, factor[home], 0.0)
            for tile in lines:
                entry = jnp.broadcast_to(tile[home][place : place + 1, :], (8, 128))
                for v in below:
                    tile[v] = tile[v] - factor[v] * entry
    scale = [lax.rsqrt(pivot) for pivot in pivots]
    return [
        jnp.concatenate([line * by for line, by in zip(tile, scale)], axis=0) for tile in lines
    ]


def factor_inverse(work, feat):
    count = LEAF // 8
    for start in range(0, feat, LEAF):
        stop = start + LEAF
        first = start // 128
        tiles = list(range(first, feat // 128 + (stop - 1) // 128 + 1))
        lines = [
            [work[start + 8 * v : start + 8 * v + 8, 128 * t : 128 * t + 128] for v in range(count)]
            for t in tiles
        ]
        done = jnp.concatenate(factor_rows(lines, start - 128 * first), axis=1)
        work[start:stop, 128 * first : 128 * (tiles[-1] + 1)] = done
        if stop < feat:
            high, mid, low = thirds(done)
            left = jnp.concatenate([high, high, mid, high, mid, low], axis=0)
            right = jnp.concatenate([high, mid, high, low, mid, high], axis=0)
            span = slice(128 * (stop // 128), 128 * (tiles[-1] + 1))
            skip = span.start - 128 * first
            for top, bottom in ((stop, stop + LEAF), (stop + LEAF, feat)):
                if top < bottom:
                    update = lax.dot_general(
                        left[:, top - 128 * first : bottom - 128 * first],
                        right[:, skip:],
                        (((0,), (0,)), ((), ())),
                        preferred_element_type=jnp.float32,
                    )
                    work[top:bottom, span] = work[top:bottom, span] - update


def layout(feat):
    tops = range(0, feat, 256)
    sides = [(top, side) for top in range(0, feat, 128) for side in range(top + 128, feat, 128)]
    pair_at = {top: top // 2 for top in tops}
    side_at = {pair: feat // 2 + 128 * place for place, pair in enumerate(sides)}
    return tops, sides, pair_at, side_at, feat // 2 + 128 * len(sides)


def far_first(index, count, turn):
    if count % 2:
        return lax.rem(index + 1 + turn, count)
    half = count // 2
    mine = lax.div(index, half) * half
    other = half - mine
    return jnp.where(
        turn < half,
        other + lax.rem(index + half // 2 + turn, half),
        mine + lax.rem(index + 1 + turn, half),
    )


def ends_first(index, count, turn, shift=0):
    if count % 4:
        return far_first(index, count, turn)
    half = count // 2
    block = count // 4
    mine = lax.div(index, half) * half
    step = lax.div(turn, block)
    end = jnp.where(index < half, 3 - step, step) * block
    across = end + lax.rem(index + shift + turn, block)
    return jnp.where(turn < half, across, mine + lax.rem(index + 1 + turn, half))


def kernel(
    n_dom,
    n_sub,
    near_each,
    features_in,
    weight_in,
    far_in,
    near_in,
    dst_in,
    inner_in,
    outer_in,
    live_in,
    tile_in,
    hidden_ref,
    inverse_ref,
    sums_ref,
    features_ref,
    weight_ref,
    far_ref,
    near_ref,
    dst_ref,
    inner_ref,
    outer_ref,
    live_ref,
    tile_ref,
    far_send,
    near_send,
    arrived,
    table,
    products,
    acc,
    aggregate,
    features_t,
    part,
    part_in,
    part_own,
    whole,
    work,
    load_sems,
    halo_sems,
    sum_sems,
):
    total_devices = n_dom * n_sub
    dom = lax.axis_index("dom")
    sub = lax.axis_index("sub")
    me = dom * n_sub + sub
    tiles, size, feat = features_ref.shape
    rows = tiles * size
    slots = inner_ref.shape[0]
    share = part_own.shape[1]
    owners = part.shape[1] // share
    first_owner = (total_devices - owners) // 2
    mine = me - first_owner
    owns = jnp.logical_and(mine >= 0, mine < owners)

    def share_rows(owner):
        return pl.ds(pl.multiple_of(owner * share, share), share)

    def device_of(index):
        return (lax.div(index, n_sub), lax.rem(index, n_sub))

    incoming = (
        (far_in, far_ref),
        (near_in, near_ref),
        (features_in, features_ref),
        (inner_in, inner_ref),
        (outer_in, outer_ref),
        (dst_in, dst_ref),
        (live_in, live_ref),
        (tile_in, tile_ref),
        (weight_in, weight_ref),
    )
    loads = [
        pltpu.make_async_copy(source, target, load_sems.at[place])
        for place, (source, target) in enumerate(incoming)
    ]

    barrier = pltpu.get_barrier_semaphore()

    for load in loads[:3]:
        load.start()

    @pl.loop(1, n_dom)
    def _(offset):
        peer = lax.rem(dom + offset, n_dom)
        pl.semaphore_signal(barrier, inc=1, device_id=(peer, sub), device_id_type=MESH)

    @pl.loop(1, n_sub)
    def _(offset):
        peer = lax.rem(sub + offset, n_sub)
        pl.semaphore_signal(barrier, inc=1, device_id=(dom, peer), device_id_type=MESH)

    for load in loads[3:]:
        load.start()
    for load in loads[:3]:
        load.wait()

    features = features_ref[...].reshape(rows, feat)

    def gather(index_row):
        return jnp.dot(
            one_hot_rows(index_row, rows), features, preferred_element_type=jnp.float32
        ).astype(jnp.bfloat16)

    far_half = far_send.shape[0] // 2
    halved = n_dom % 4 == 0 and far_half % 128 == 0
    across_first = pl.multiple_of(jnp.where(dom < n_dom // 2, far_half, 0), far_half)
    inside_first = pl.multiple_of(far_half - across_first, far_half)
    if halved:
        far_send[pl.ds(across_first, far_half), :] = gather(far_ref[:, pl.ds(across_first, far_half)])
    else:
        far_send[...] = gather(far_ref[...])
        near_send[...] = gather(near_ref[...])
    per_dom = far_send.shape[0] // n_dom
    per_sub = near_send.shape[0] // n_sub
    far_count = per_dom * n_dom
    packed = size % per_dom == 0 and size % per_sub == 0 and arrived.shape[0] == table.shape[0] * size

    def place(first, count):
        if packed:
            within = pl.multiple_of(lax.rem(first, size), count)
            return table.at[lax.div(first, size), pl.ds(within, count)]
        return arrived.at[pl.ds(pl.multiple_of(first, count), count)]

    def dom_rows(index):
        return pl.ds(pl.multiple_of(index * per_dom, per_dom), per_dom)

    def sub_rows(index):
        return pl.ds(pl.multiple_of(index * per_sub, per_sub), per_sub)

    def dom_place(index):
        return place(index * per_dom, per_dom)

    def sub_place(index):
        return place(far_count + index * per_sub, per_sub)

    pl.semaphore_wait(barrier, n_dom + n_sub - 2)

    def send_far(turn):
        peer = ends_first(dom, n_dom, turn, 0)
        pltpu.make_async_remote_copy(
            src_ref=far_send.at[dom_rows(peer)],
            dst_ref=dom_place(dom),
            send_sem=halo_sems.at[0],
            recv_sem=halo_sems.at[1],
            device_id=(peer, sub),
            device_id_type=MESH,
        ).start()

    if halved:
        pl.loop(0, n_dom // 2)(send_far)
        far_send[pl.ds(inside_first, far_half), :] = gather(far_ref[:, pl.ds(inside_first, far_half)])
        pl.loop(n_dom // 2, n_dom - 1)(send_far)
        near_send[...] = gather(near_ref[...])
    else:
        pl.loop(0, n_dom - 1)(send_far)

    @pl.loop(0, n_sub - 1)
    def _(turn):
        peer = far_first(sub, n_sub, turn)
        pltpu.make_async_remote_copy(
            src_ref=near_send.at[sub_rows(peer)],
            dst_ref=sub_place(sub),
            send_sem=halo_sems.at[2],
            recv_sem=halo_sems.at[3],
            device_id=(dom, peer),
            device_id_type=MESH,
        ).start()

    dom_place(dom)[...] = far_send[dom_rows(dom), :]
    sub_place(sub)[...] = near_send[sub_rows(sub), :]

    def slot_products(rows_ref, source, first):
        for slot in range(slots):
            products[slot] = jnp.dot(
                tile_ref[first + slot],
                rows_ref[source[slot]],
                preferred_element_type=jnp.float32,
            )

    def slot_sum(tile, first, count):
        total = None
        for slot in range(slots):
            target = jnp.full((1, feat), dst_ref[first + slot], jnp.int32)
            chosen = jnp.where(jnp.logical_and(target == tile, count > slot), 1.0, 0.0)
            term = products[slot] * chosen
            total = term if total is None else total + term
        return total

    for load in loads[3:]:
        load.wait()
    slot_products(features_ref, inner_ref, 0)
    features_t[...] = features.T
    squares = features.astype(jnp.float32)
    squares = jnp.sum(squares * squares, axis=0, keepdims=True)
    square_row = squares[:, :128]
    for side in range(128, feat, 128):
        square_row = square_row + squares[:, side : side + 128]
    inner_count = jnp.full((1, feat), live_ref[0, 0], jnp.int32)
    outer_count = jnp.full((1, feat), live_ref[0, 1], jnp.int32)

    @pl.loop(0, tiles)
    def _(tile):
        acc[tile] = slot_sum(tile, 0, inner_count)

    def settle(ref, sem):
        pltpu.make_async_copy(ref, ref, sem).wait()

    settle(arrived.at[pl.ds(0, per_dom * (n_dom - 1))], halo_sems.at[1])
    settle(arrived.at[pl.ds(0, per_sub * (n_sub - 1))], halo_sems.at[3])
    if not packed:
        table[...] = jnp.dot(
            packing(table.shape[0] * size, arrived.shape[0], n_dom, n_sub, per_dom, per_sub, near_each),
            arrived[...],
            preferred_element_type=jnp.float32,
        ).astype(jnp.bfloat16).reshape(table.shape)
    slot_products(table, outer_ref, slots)

    @pl.loop(0, tiles)
    def _(tile):
        total = acc[tile] + slot_sum(tile, slots, outer_count)
        aggregate[pl.ds(pl.multiple_of(tile * size, size), size), :] = total.astype(jnp.bfloat16)

    projected = jnp.dot(aggregate[...], weight_ref[...], preferred_element_type=jnp.float32)
    hidden = (
        features_ref[...].reshape(rows, feat).astype(jnp.float32) + projected / (1.0 + jnp.exp(-projected))
    ).astype(jnp.bfloat16)
    hidden_ref[...] = hidden
    hidden_t = hidden.T
    row = lax.broadcasted_iota(jnp.int32, (128, 128), 0)
    lane = lax.broadcasted_iota(jnp.int32, (128, 128), 1)
    tops, sides, pair_at, side_at, extra_at = layout(feat)

    def diagonal_row(block):
        return jnp.sum(jnp.where(row == lane, block, 0.0), axis=0, keepdims=True)

    def send_parts(kind):
        half = owners // 2
        left = me < total_devices // 2
        first_count = jnp.where(left, owners - half, half)
        first_base = jnp.where(left, half, 0)
        last_count = owners - first_count
        last_base = half - first_base

        @pl.loop(0, owners)
        def _(turn):
            owner = jnp.where(
                turn < first_count,
                first_base + lax.rem(me + turn, first_count),
                last_base + lax.rem(me + turn, last_count),
            )
            peer = first_owner + owner

            @pl.when(peer != me)
            def _():
                pltpu.make_async_remote_copy(
                    src_ref=part.at[kind, share_rows(owner)],
                    dst_ref=part_in.at[kind, me],
                    send_sem=sum_sems.at[4 * kind],
                    recv_sem=sum_sems.at[4 * kind + 1],
                    device_id=device_of(peer),
                    device_id_type=MESH,
                ).start()

    def share_sum(kind):
        @pl.when(owns)
        def _():
            part_in[kind, me] = part[kind, share_rows(mine), :]
            settle(part_in.at[kind, pl.ds(0, total_devices - 1)], sum_sems.at[4 * kind + 1])
            total = jnp.sum(part_in[kind], axis=0)
            part_own[kind] = total
            whole[kind, share_rows(mine), :] = total

            @pl.loop(0, total_devices - 1)
            def _(turn):
                peer = far_first(me, total_devices, turn)
                pltpu.make_async_remote_copy(
                    src_ref=part_own.at[kind],
                    dst_ref=whole.at[kind, share_rows(mine)],
                    send_sem=sum_sems.at[4 * kind + 2],
                    recv_sem=sum_sems.at[4 * kind + 3],
                    device_id=device_of(peer),
                    device_id_type=MESH,
                ).start()

    def await_sum(kind):
        @pl.when(owns)
        def _():
            settle(whole.at[kind, pl.ds(0, share * (owners - 1))], sum_sems.at[4 * kind + 3])

        @pl.when(jnp.logical_not(owns))
        def _():
            settle(whole.at[kind], sum_sems.at[4 * kind + 3])

    def await_sends(kind):
        @pl.when(owns)
        def _():
            settle(part.at[kind, pl.ds(0, share * (owners - 1))], sum_sems.at[4 * kind])
            settle(part_in.at[kind, pl.ds(0, total_devices - 1)], sum_sems.at[4 * kind + 2])

        @pl.when(jnp.logical_not(owns))
        def _():
            settle(part.at[kind], sum_sems.at[4 * kind])

    part[:, extra_at:, :] = jnp.zeros((2, part.shape[1] - extra_at, 128), jnp.float32)
    stripes = {
        top: jnp.dot(hidden_t[top : top + 128, :], hidden[:, top:], preferred_element_type=jnp.float32)
        for top in range(0, feat, 128)
    }
    for top in tops:
        low = stripes[top + 128][:, :128]
        part[0, pair_at[top] : pair_at[top] + 128, :] = jnp.where(row <= lane, stripes[top][:, :128], low)
        place = extra_at + top // 256
        part[0, place : place + 1, :] = diagonal_row(low)
    for top, side in sides:
        at = side_at[top, side]
        part[0, at : at + 128, :] = stripes[top][:, side - top : side - top + 128]
    send_parts(0)

    for top in tops:
        stripe = jnp.dot(
            features_t[top:, :], hidden[:, top : top + 128], preferred_element_type=jnp.float32
        )
        low = jnp.dot(
            hidden_t[top + 128 : top + 256, :],
            features_ref[...].reshape(rows, feat)[:, top + 128 : top + 256],
            preferred_element_type=jnp.float32,
        )
        part[1, pair_at[top] : pair_at[top] + 128, :] = jnp.where(row >= lane, stripe[:128, :], low)
        place = extra_at + top // 256
        part[1, place : place + 1, :] = diagonal_row(low)
        for side in range(top + 128, feat, 128):
            at = side_at[top, side]
            part[1, at : at + 128, :] = stripe[side - top : side - top + 128, :]
    for top in range(128, feat, 256):
        for side in range(top + 128, feat, 128):
            at = side_at[top, side]
            part[1, at : at + 128, :] = jnp.dot(
                features_t[side : side + 128, :],
                hidden[:, top : top + 128],
                preferred_element_type=jnp.float32,
            )
    square_at = extra_at + feat // 256
    part[1, square_at : square_at + 1, :] = square_row
    send_parts(1)
    share_sum(0)
    share_sum(1)
    await_sum(0)

    vertex_count = rows * total_devices
    diagonal = lax.broadcasted_iota(jnp.int32, (feat, feat), 0) == lax.broadcasted_iota(
        jnp.int32, (feat, feat), 1
    )
    identity = jnp.where(diagonal, 1.0, 0.0)
    inner_identity = epsilon * identity[:128, :128]
    for top in tops:
        pair = whole[0, pair_at[top] : pair_at[top] + 128, :] / vertex_count
        turned = pair.T
        place = extra_at + top // 256
        low_diagonal = whole[0, place : place + 1, :] / vertex_count
        work[top : top + 128, top : top + 128] = jnp.where(row <= lane, pair, turned) + inner_identity
        low = jnp.where(row == lane, low_diagonal, jnp.where(row > lane, pair, turned))
        work[top + 128 : top + 256, top + 128 : top + 256] = low + inner_identity
    for top, side in sides:
        at = side_at[top, side]
        work[top : top + 128, side : side + 128] = whole[0, at : at + 128, :] / vertex_count
        work[side : side + 128, top : top + 128] = jnp.zeros((128, 128), jnp.float32)
    work[:, feat:] = identity
    factor_inverse(work, feat)

    inverse_ref[...] = work[:, feat:]

    settle(far_send.at[pl.ds(0, per_dom * (n_dom - 1))], halo_sems.at[0])
    settle(near_send.at[pl.ds(0, per_sub * (n_sub - 1))], halo_sems.at[2])

    await_sends(0)
    await_sends(1)
    await_sum(1)
    sums_ref[...] = whole[1]


def whiten(vertex_count, hidden_ref, inverse_ref, sums_ref, out_ref, loss_ref, result, sems):
    rows = hidden_ref.shape[0]
    across = (((1,), (1,)), ((), ()))
    step = rows // CHUNKS
    stores = []
    inverse = inverse_ref[...]
    high_part = inverse.astype(jnp.bfloat16)
    low_part = (inverse - high_part.astype(jnp.float32)).astype(jnp.bfloat16)
    for chunk in range(CHUNKS):
        here = pl.ds(chunk * step, step)
        hidden = hidden_ref[here, :]
        white = lax.dot_general(
            hidden, high_part, across, preferred_element_type=jnp.float32
        ) + lax.dot_general(hidden, low_part, across, preferred_element_type=jnp.float32)
        result[here, :] = white.astype(jnp.bfloat16)
        store = pltpu.make_async_copy(result.at[here], out_ref.at[here], sems.at[chunk])
        store.start()
        stores.append(store)
    feat = hidden_ref.shape[1]
    tops, sides, pair_at, side_at, extra_at = layout(feat)
    squares = extra_at + feat // 256
    row = lax.broadcasted_iota(jnp.int32, (128, 128), 0)
    lane = lax.broadcasted_iota(jnp.int32, (128, 128), 1)
    cross = jnp.zeros((128, 128), jnp.float32)
    norm = jnp.zeros((128, 128), jnp.float32)
    for top in tops:
        upper = inverse_ref[top : top + 128, top : top + 128]
        lower = inverse_ref[top + 128 : top + 256, top + 128 : top + 256]
        place = extra_at + top // 256
        pair = sums_ref[pair_at[top] : pair_at[top] + 128, :]
        low_diagonal = sums_ref[place : place + 1, :]
        cross = cross + jnp.where(row >= lane, upper, lower.T) * pair
        cross = cross + jnp.where(row == lane, lower * low_diagonal, 0.0)
        norm = norm + upper * upper + lower * lower
    for top, side in sides:
        at = side_at[top, side]
        across_block = inverse_ref[side : side + 128, top : top + 128]
        cross = cross + across_block * sums_ref[at : at + 128, :]
        norm = norm + across_block * across_block
    rest = jnp.sum(-2.0 * cross - (vertex_count * epsilon) * norm, axis=0, keepdims=True)
    rest = rest + sums_ref[squares : squares + 1, :]
    loss_ref[0, 0] = 1.0 + jnp.sum(rest) / (vertex_count * feat)
    for store in stores:
        store.wait()


def body(
    n_dom,
    n_sub,
    features,
    weight,
    send_far,
    send_near,
    tile_dst,
    inner_src,
    outer_src,
    tile_live,
    tile_weight,
):
    rows, feat = features.shape
    size = tile_weight.shape[1]
    slots = inner_src.shape[0]
    total = n_dom * n_sub
    wide = feat // 128
    extra = feat // 256 + 1
    packed_rows = feat // 2 + 64 * wide * (wide - 1) + extra
    share = 8
    while -(-packed_rows // share) > total // 2 + 1:
        share += 8
    packed_rows = -(-packed_rows // share) * share
    far_count = send_far.shape[0]
    near_count = send_near.shape[0]

    def padded(index, peers):
        each = index.shape[0] // peers
        grid = index.reshape(peers, each)
        return jnp.pad(grid, ((0, 0), (0, padded_rows(each) - each))).reshape(1, -1)

    far_index = padded(send_far, n_dom)
    near_index = padded(send_near, n_sub)
    far_padded = far_index.shape[1]
    near_padded = near_index.shape[1]
    anywhere = pl.BlockSpec(memory_space=pltpu.HBM)
    smem = pl.BlockSpec(memory_space=pltpu.SMEM)
    f32 = jnp.float32
    bf16 = jnp.bfloat16
    vmem = pl.BlockSpec(memory_space=pltpu.VMEM)
    hidden, inverse, sums = pl.pallas_call(
        functools.partial(kernel, n_dom, n_sub, near_count // n_sub),
        out_shape=(
            pltpu.VMEM((rows, feat), bf16),
            pltpu.VMEM((feat, feat), f32),
            pltpu.VMEM((packed_rows, 128), f32),
        ),
        in_specs=[anywhere] * 9,
        out_specs=(vmem, vmem, vmem),
        scratch_shapes=[
            pltpu.VMEM((rows // size, size, feat), bf16),
            pltpu.VMEM(weight.shape, bf16),
            pltpu.VMEM((1, far_padded), jnp.int32),
            pltpu.VMEM((1, near_padded), jnp.int32),
            pltpu.SMEM(tile_dst.shape, jnp.int32),
            pltpu.SMEM(inner_src.shape, jnp.int32),
            pltpu.SMEM(outer_src.shape, jnp.int32),
            pltpu.SMEM(tile_live.shape, jnp.int32),
            pltpu.VMEM(tile_weight.shape, bf16),
            pltpu.VMEM((far_padded, feat), bf16),
            pltpu.VMEM((near_padded, feat), bf16),
            pltpu.VMEM((far_padded + near_padded, feat), bf16),
            pltpu.VMEM(((far_count + near_count) // size, size, feat), bf16),
            pltpu.VMEM((slots, size, feat), f32),
            pltpu.VMEM((rows // size, size, feat), f32),
            pltpu.VMEM((rows, feat), bf16),
            pltpu.VMEM((feat, rows), bf16),
            pltpu.VMEM((2, packed_rows, 128), f32),
            pltpu.VMEM((2, total, share, 128), f32),
            pltpu.VMEM((2, share, 128), f32),
            pltpu.VMEM((2, packed_rows, 128), f32),
            pltpu.VMEM((feat, 2 * feat), f32),
            pltpu.SemaphoreType.DMA((10,)),
            pltpu.SemaphoreType.DMA((4,)),
            pltpu.SemaphoreType.DMA((8,)),
        ],
        compiler_params=pltpu.CompilerParams(
            collective_id=0, has_side_effects=True, vmem_limit_bytes=VMEM_LIMIT
        ),
    )(
        *[
            pltpu.with_memory_space_constraint(value, pltpu.HBM)
            for value in (
                features.reshape(rows // size, size, feat),
                weight,
                far_index,
                near_index,
                tile_dst,
                inner_src,
                outer_src,
                tile_live,
                tile_weight,
            )
        ]
    )
    whitened, loss = pl.pallas_call(
        functools.partial(whiten, rows * total),
        out_shape=(
            jax.ShapeDtypeStruct((rows, feat), bf16),
            jax.ShapeDtypeStruct((1, 1), f32),
        ),
        in_specs=[vmem, vmem, vmem],
        out_specs=(anywhere, smem),
        scratch_shapes=[pltpu.VMEM((rows, feat), bf16), pltpu.SemaphoreType.DMA((CHUNKS,))],
        compiler_params=pltpu.CompilerParams(vmem_limit_bytes=VMEM_LIMIT),
    )(hidden, inverse, sums)
    return whitened, loss.reshape(())


def solution(mesh):
    placed = (
        P(("dom", "sub"), None),
        P(),
        P(("dom", "sub")),
        P(("dom", "sub")),
        P(("dom", "sub")),
        P(("dom", "sub")),
        P(("dom", "sub")),
        P(("dom", "sub"), None),
        P(("dom", "sub"), None, None),
    )
    return jax.shard_map(
        functools.partial(body, mesh.shape["dom"], mesh.shape["sub"]),
        mesh=mesh,
        in_specs=placed,
        out_specs=(P(("dom", "sub"), None), P()),
        check_vma=False,
    )
```

```python
import functools

import jax
import jax.numpy as jnp
from jax import lax
from jax.experimental import pallas as pl
from jax.experimental.pallas import tpu as pltpu
from jax.sharding import PartitionSpec as P

epsilon = 1e-05
MESH = pl.DeviceIdType.MESH
LEAF = 32
GROUP = 16
CHUNKS = 4
UNROLL = 8
VMEM_LIMIT = 32 * 1024 * 1024


def one_hot_rows(index_row, row_count):
    rows = index_row.shape[1]
    columns = jnp.broadcast_to(index_row, (128, rows)).T
    lane = lax.broadcasted_iota(jnp.int32, (rows, 128), 1)
    parts = [
        jnp.where(columns == lane + start, 1.0, 0.0).astype(jnp.bfloat16)
        for start in range(0, row_count, 128)
    ]
    return jnp.concatenate(parts, axis=1)


def padded_rows(count):
    return -(-count // 16) * 16


def packing(packed_rows, padded_total, n_dom, n_sub, per_dom, per_sub, near_rows_each):
    near_total = n_sub * near_rows_each
    far_total = packed_rows - near_total
    far_rows_each = far_total // n_dom
    row = lax.broadcasted_iota(jnp.int32, (packed_rows, padded_total), 0)
    column = lax.broadcasted_iota(jnp.int32, (packed_rows, padded_total), 1)
    far_place = row + lax.div(row, far_rows_each) * (per_dom - far_rows_each)
    near_row = row - far_total
    near_place = (
        n_dom * per_dom + near_row + lax.div(near_row, near_rows_each) * (per_sub - near_rows_each)
    )
    place = jnp.where(row < far_total, far_place, near_place)
    return jnp.where(place == column, 1.0, 0.0).astype(jnp.bfloat16)


def thirds(block):
    high = block.astype(jnp.bfloat16)
    rest = block - high.astype(jnp.float32)
    mid = rest.astype(jnp.bfloat16)
    low = (rest - mid.astype(jnp.float32)).astype(jnp.bfloat16)
    return high, mid, low


def factor_rows(lines, lanes):
    count = len(lines[0])
    sub = lax.broadcasted_iota(jnp.int32, (8, 128), 0)
    pivots = [jnp.zeros((8, 128), jnp.float32)] * count
    for start in range(0, 8 * count, GROUP):
        tall = range(start // 8, count)
        columns = []
        for k in range(start, start + GROUP):
            tile, lane = divmod(lanes + k, 128)
            columns.append({
                v: jnp.broadcast_to(lines[tile][v][:, lane : lane + 1], (8, 128)) for v in tall
            })
        for i in range(GROUP):
            home, place = divmod(start + i, 8)
            pivot = jnp.broadcast_to(columns[i][home][place : place + 1, :], (8, 128))
            pivots[home] = jnp.where(sub == place, pivot, pivots[home])
            inverse = 1.0 / pivot
            below = range(home, count)
            factor = {v: columns[i][v] * inverse for v in below}
            for k in range(i + 1, GROUP):
                entry = jnp.broadcast_to(columns[k][home][place : place + 1, :], (8, 128))
                for v in below:
                    columns[k][v] = columns[k][v] - factor[v] * entry
            factor[home] = jnp.where(sub > place, factor[home], 0.0)
            for tile in lines:
                entry = jnp.broadcast_to(tile[home][place : place + 1, :], (8, 128))
                for v in below:
                    tile[v] = tile[v] - factor[v] * entry
    scale = [lax.rsqrt(pivot) for pivot in pivots]
    return [
        jnp.concatenate([line * by for line, by in zip(tile, scale)], axis=0) for tile in lines
    ]


def factor_inverse(work, feat, between):
    count = LEAF // 8
    for start in range(0, feat, LEAF):
        if start == LEAF:
            between()
        stop = start + LEAF
        first = start // 128
        tiles = list(range(first, feat // 128 + (stop - 1) // 128 + 1))
        lines = [
            [work[start + 8 * v : start + 8 * v + 8, 128 * t : 128 * t + 128] for v in range(count)]
            for t in tiles
        ]
        done = jnp.concatenate(factor_rows(lines, start - 128 * first), axis=1)
        work[start:stop, 128 * first : 128 * (tiles[-1] + 1)] = done
        if stop < feat:
            high, mid, low = thirds(done)
            left = jnp.concatenate([high, high, mid, high, mid, low], axis=0)
            right = jnp.concatenate([high, mid, high, low, mid, high], axis=0)
            span = slice(128 * (stop // 128), 128 * (tiles[-1] + 1))
            skip = span.start - 128 * first
            for top, bottom in ((stop, stop + LEAF), (stop + LEAF, feat)):
                if top < bottom:
                    update = lax.dot_general(
                        left[:, top - 128 * first : bottom - 128 * first],
                        right[:, skip:],
                        (((0,), (0,)), ((), ())),
                        preferred_element_type=jnp.float32,
                    )
                    work[top:bottom, span] = work[top:bottom, span] - update


def layout(feat):
    tops = range(0, feat, 256)
    sides = [(top, side) for top in range(0, feat, 128) for side in range(top + 128, feat, 128)]
    pair_at = {top: top // 2 for top in tops}
    side_at = {pair: feat // 2 + 128 * place for place, pair in enumerate(sides)}
    return tops, sides, pair_at, side_at, feat // 2 + 128 * len(sides)


def each(count, step):
    whole, rest = divmod(count, UNROLL)
    if whole > 1:

        @pl.loop(0, whole)
        def _(turn):
            for place in range(UNROLL):
                step(turn * UNROLL + place)
    elif whole:
        rest = count
        whole = 0
    for place in range(rest):
        step(whole * UNROLL + place)


def far_first(index, count, turn):
    if count % 2:
        return lax.rem(index + 1 + turn, count)
    half = count // 2
    mine = lax.div(index, half) * half
    other = half - mine
    return jnp.where(
        turn < half,
        other + lax.rem(index + half // 2 + turn, half),
        mine + lax.rem(index + 1 + turn, half),
    )


def ends_first(index, count, turn, shift=0):
    if count % 4:
        return far_first(index, count, turn)
    half = count // 2
    block = count // 4
    mine = lax.div(index, half) * half
    step = lax.div(turn, block)
    end = jnp.where(index < half, 3 - step, step) * block
    across = end + lax.rem(index + shift + turn, block)
    return jnp.where(turn < half, across, mine + lax.rem(index + 1 + turn, half))


def kernel(
    n_dom,
    n_sub,
    near_each,
    features_in,
    weight_in,
    far_in,
    near_in,
    dst_in,
    inner_in,
    outer_in,
    live_in,
    tile_in,
    hidden_ref,
    inverse_ref,
    sums_ref,
    features_ref,
    weight_ref,
    far_ref,
    near_ref,
    dst_ref,
    inner_ref,
    outer_ref,
    live_ref,
    tile_ref,
    far_send,
    near_send,
    arrived,
    table,
    products,
    acc,
    aggregate,
    features_t,
    part,
    part_in,
    part_own,
    whole,
    work,
    load_sems,
    halo_sems,
    sum_sems,
):
    total_devices = n_dom * n_sub
    dom = lax.axis_index("dom")
    sub = lax.axis_index("sub")
    me = dom * n_sub + sub
    tiles, size, feat = features_ref.shape
    rows = tiles * size
    slots = inner_ref.shape[0]
    share = part_own.shape[1]
    owners = part.shape[1] // share
    first_owner = (total_devices - owners) // 2
    mine = me - first_owner
    owns = jnp.logical_and(mine >= 0, mine < owners)

    def share_rows(owner):
        return pl.ds(pl.multiple_of(owner * share, share), share)

    def device_of(index):
        return (lax.div(index, n_sub), lax.rem(index, n_sub))

    incoming = (
        (far_in, far_ref),
        (near_in, near_ref),
        (features_in, features_ref),
        (inner_in, inner_ref),
        (outer_in, outer_ref),
        (dst_in, dst_ref),
        (live_in, live_ref),
        (tile_in, tile_ref),
        (weight_in, weight_ref),
    )
    loads = [
        pltpu.make_async_copy(source, target, load_sems.at[place])
        for place, (source, target) in enumerate(incoming)
    ]

    barrier = pltpu.get_barrier_semaphore()

    for load in loads[:3]:
        load.start()

    @pl.loop(1, n_dom)
    def _(offset):
        peer = lax.rem(dom + offset, n_dom)
        pl.semaphore_signal(barrier, inc=1, device_id=(peer, sub), device_id_type=MESH)

    @pl.loop(1, n_sub)
    def _(offset):
        peer = lax.rem(sub + offset, n_sub)
        pl.semaphore_signal(barrier, inc=1, device_id=(dom, peer), device_id_type=MESH)

    for load in loads[3:]:
        load.start()
    loads[0].wait()
    loads[1].wait()
    far_half = far_send.shape[0] // 2
    halved = n_dom % 4 == 0 and far_half % 128 == 0
    across_first = pl.multiple_of(jnp.where(dom < n_dom // 2, far_half, 0), far_half)
    inside_first = pl.multiple_of(far_half - across_first, far_half)
    if halved:
        across_picks = one_hot_rows(far_ref[:, pl.ds(across_first, far_half)], rows)
    loads[2].wait()
    features = features_ref[...].reshape(rows, feat)

    def gather(picks):
        return jnp.dot(picks, features, preferred_element_type=jnp.float32).astype(jnp.bfloat16)

    if halved:
        far_send[pl.ds(across_first, far_half), :] = gather(across_picks)
    else:
        far_send[...] = gather(one_hot_rows(far_ref[...], rows))
        near_send[...] = gather(one_hot_rows(near_ref[...], rows))
    per_dom = far_send.shape[0] // n_dom
    per_sub = near_send.shape[0] // n_sub
    far_count = per_dom * n_dom
    packed = size % per_dom == 0 and size % per_sub == 0 and arrived.shape[0] == table.shape[0] * size

    def place(first, count):
        if packed:
            within = pl.multiple_of(lax.rem(first, size), count)
            return table.at[lax.div(first, size), pl.ds(within, count)]
        return arrived.at[pl.ds(pl.multiple_of(first, count), count)]

    def dom_rows(index):
        return pl.ds(pl.multiple_of(index * per_dom, per_dom), per_dom)

    def sub_rows(index):
        return pl.ds(pl.multiple_of(index * per_sub, per_sub), per_sub)

    def dom_place(index):
        return place(index * per_dom, per_dom)

    def sub_place(index):
        return place(far_count + index * per_sub, per_sub)

    pl.semaphore_wait(barrier, n_dom + n_sub - 2)

    def send_far(turn):
        peer = ends_first(dom, n_dom, turn, 0)
        pltpu.make_async_remote_copy(
            src_ref=far_send.at[dom_rows(peer)],
            dst_ref=dom_place(dom),
            send_sem=halo_sems.at[0],
            recv_sem=halo_sems.at[1],
            device_id=(peer, sub),
            device_id_type=MESH,
        ).start()

    if halved:
        each(n_dom // 2, send_far)
        far_send[pl.ds(inside_first, far_half), :] = gather(one_hot_rows(far_ref[:, pl.ds(inside_first, far_half)], rows))
        pl.loop(n_dom // 2, n_dom - 1)(send_far)
        near_send[...] = gather(one_hot_rows(near_ref[...], rows))
    else:
        pl.loop(0, n_dom - 1)(send_far)

    @pl.loop(0, n_sub - 1)
    def _(turn):
        peer = far_first(sub, n_sub, turn)
        pltpu.make_async_remote_copy(
            src_ref=near_send.at[sub_rows(peer)],
            dst_ref=sub_place(sub),
            send_sem=halo_sems.at[2],
            recv_sem=halo_sems.at[3],
            device_id=(dom, peer),
            device_id_type=MESH,
        ).start()

    dom_place(dom)[...] = far_send[dom_rows(dom), :]
    sub_place(sub)[...] = near_send[sub_rows(sub), :]

    def slot_products(rows_ref, source, first):
        for slot in range(slots):
            products[slot] = jnp.dot(
                tile_ref[first + slot],
                rows_ref[source[slot]],
                preferred_element_type=jnp.float32,
            )

    def slot_sum(tile, first, count):
        total = None
        for slot in range(slots):
            target = jnp.full((1, feat), dst_ref[first + slot], jnp.int32)
            chosen = jnp.where(jnp.logical_and(target == tile, count > slot), 1.0, 0.0)
            term = products[slot] * chosen
            total = term if total is None else total + term
        return total

    for load in loads[3:]:
        load.wait()
    slot_products(features_ref, inner_ref, 0)
    features_t[...] = features.T
    squares = features.astype(jnp.float32)
    squares = jnp.sum(squares * squares, axis=0, keepdims=True)
    square_row = squares[:, :128]
    for side in range(128, feat, 128):
        square_row = square_row + squares[:, side : side + 128]
    inner_count = jnp.full((1, feat), live_ref[0, 0], jnp.int32)
    outer_count = jnp.full((1, feat), live_ref[0, 1], jnp.int32)

    @pl.loop(0, tiles)
    def _(tile):
        acc[tile] = slot_sum(tile, 0, inner_count)

    def settle(ref, sem):
        pltpu.make_async_copy(ref, ref, sem).wait()

    settle(arrived.at[pl.ds(0, per_dom * (n_dom - 1))], halo_sems.at[1])
    settle(arrived.at[pl.ds(0, per_sub * (n_sub - 1))], halo_sems.at[3])
    if not packed:
        table[...] = jnp.dot(
            packing(table.shape[0] * size, arrived.shape[0], n_dom, n_sub, per_dom, per_sub, near_each),
            arrived[...],
            preferred_element_type=jnp.float32,
        ).astype(jnp.bfloat16).reshape(table.shape)
    slot_products(table, outer_ref, slots)

    @pl.loop(0, tiles)
    def _(tile):
        total = acc[tile] + slot_sum(tile, slots, outer_count)
        aggregate[pl.ds(pl.multiple_of(tile * size, size), size), :] = total.astype(jnp.bfloat16)

    projected = jnp.dot(aggregate[...], weight_ref[...], preferred_element_type=jnp.float32)
    hidden = (
        features_ref[...].reshape(rows, feat).astype(jnp.float32) + projected / (1.0 + jnp.exp(-projected))
    ).astype(jnp.bfloat16)
    hidden_ref[...] = hidden
    hidden_t = hidden.T
    row = lax.broadcasted_iota(jnp.int32, (128, 128), 0)
    lane = lax.broadcasted_iota(jnp.int32, (128, 128), 1)
    tops, sides, pair_at, side_at, extra_at = layout(feat)

    def diagonal_row(block):
        return jnp.sum(jnp.where(row == lane, block, 0.0), axis=0, keepdims=True)

    def send_parts(kind):
        half = owners // 2
        left = me < total_devices // 2
        first_count = jnp.where(left, owners - half, half)
        first_base = jnp.where(left, half, 0)
        last_count = owners - first_count
        last_base = half - first_base

        def send(turn):
            owner = jnp.where(
                turn < first_count,
                first_base + lax.rem(me + turn, first_count),
                last_base + lax.rem(me + turn, last_count),
            )
            peer = first_owner + owner

            @pl.when(peer != me)
            def _():
                pltpu.make_async_remote_copy(
                    src_ref=part.at[kind, share_rows(owner)],
                    dst_ref=part_in.at[kind, me],
                    send_sem=sum_sems.at[4 * kind],
                    recv_sem=sum_sems.at[4 * kind + 1],
                    device_id=device_of(peer),
                    device_id_type=MESH,
                ).start()

        each(owners, send)

    def share_sum(kind):
        @pl.when(owns)
        def _():
            part_in[kind, me] = part[kind, share_rows(mine), :]
            settle(part_in.at[kind, pl.ds(0, total_devices - 1)], sum_sems.at[4 * kind + 1])
            total = jnp.sum(part_in[kind], axis=0)
            part_own[kind] = total
            whole[kind, share_rows(mine), :] = total

            def send(turn):
                peer = far_first(me, total_devices, turn)
                pltpu.make_async_remote_copy(
                    src_ref=part_own.at[kind],
                    dst_ref=whole.at[kind, share_rows(mine)],
                    send_sem=sum_sems.at[4 * kind + 2],
                    recv_sem=sum_sems.at[4 * kind + 3],
                    device_id=device_of(peer),
                    device_id_type=MESH,
                ).start()

            each(total_devices - 1, send)

    def await_sum(kind):
        @pl.when(owns)
        def _():
            settle(whole.at[kind, pl.ds(0, share * (owners - 1))], sum_sems.at[4 * kind + 3])

        @pl.when(jnp.logical_not(owns))
        def _():
            settle(whole.at[kind], sum_sems.at[4 * kind + 3])

    def await_sends(kind):
        @pl.when(owns)
        def _():
            settle(part.at[kind, pl.ds(0, share * (owners - 1))], sum_sems.at[4 * kind])
            settle(part_in.at[kind, pl.ds(0, total_devices - 1)], sum_sems.at[4 * kind + 2])

        @pl.when(jnp.logical_not(owns))
        def _():
            settle(part.at[kind], sum_sems.at[4 * kind])

    part[:, extra_at:, :] = jnp.zeros((2, part.shape[1] - extra_at, 128), jnp.float32)
    stripes = {
        top: jnp.dot(hidden_t[top : top + 128, :], hidden[:, top:], preferred_element_type=jnp.float32)
        for top in range(0, feat, 128)
    }
    for top in tops:
        low = stripes[top + 128][:, :128]
        part[0, pair_at[top] : pair_at[top] + 128, :] = jnp.where(row <= lane, stripes[top][:, :128], low)
        place = extra_at + top // 256
        part[0, place : place + 1, :] = diagonal_row(low)
    for top, side in sides:
        at = side_at[top, side]
        part[0, at : at + 128, :] = stripes[top][:, side - top : side - top + 128]
    send_parts(0)

    for top in tops:
        stripe = jnp.dot(
            features_t[top:, :], hidden[:, top : top + 128], preferred_element_type=jnp.float32
        )
        low = jnp.dot(
            hidden_t[top + 128 : top + 256, :],
            features_ref[...].reshape(rows, feat)[:, top + 128 : top + 256],
            preferred_element_type=jnp.float32,
        )
        part[1, pair_at[top] : pair_at[top] + 128, :] = jnp.where(row >= lane, stripe[:128, :], low)
        place = extra_at + top // 256
        part[1, place : place + 1, :] = diagonal_row(low)
        for side in range(top + 128, feat, 128):
            at = side_at[top, side]
            part[1, at : at + 128, :] = stripe[side - top : side - top + 128, :]
    for top in range(128, feat, 256):
        for side in range(top + 128, feat, 128):
            at = side_at[top, side]
            part[1, at : at + 128, :] = jnp.dot(
                features_t[side : side + 128, :],
                hidden[:, top : top + 128],
                preferred_element_type=jnp.float32,
            )
    square_at = extra_at + feat // 256
    part[1, square_at : square_at + 1, :] = square_row
    send_parts(1)
    share_sum(0)
    await_sum(0)

    vertex_count = rows * total_devices
    diagonal = lax.broadcasted_iota(jnp.int32, (feat, feat), 0) == lax.broadcasted_iota(
        jnp.int32, (feat, feat), 1
    )
    identity = jnp.where(diagonal, 1.0, 0.0)
    inner_identity = epsilon * identity[:128, :128]
    for top in tops:
        pair = whole[0, pair_at[top] : pair_at[top] + 128, :] / vertex_count
        turned = pair.T
        place = extra_at + top // 256
        low_diagonal = whole[0, place : place + 1, :] / vertex_count
        work[top : top + 128, top : top + 128] = jnp.where(row <= lane, pair, turned) + inner_identity
        low = jnp.where(row == lane, low_diagonal, jnp.where(row > lane, pair, turned))
        work[top + 128 : top + 256, top + 128 : top + 256] = low + inner_identity
    for top, side in sides:
        at = side_at[top, side]
        work[top : top + 128, side : side + 128] = whole[0, at : at + 128, :] / vertex_count
        work[side : side + 128, top : top + 128] = jnp.zeros((128, 128), jnp.float32)
    work[:, feat:] = identity
    factor_inverse(work, feat, lambda: share_sum(1))

    inverse_ref[...] = work[:, feat:]

    settle(far_send.at[pl.ds(0, per_dom * (n_dom - 1))], halo_sems.at[0])
    settle(near_send.at[pl.ds(0, per_sub * (n_sub - 1))], halo_sems.at[2])

    await_sends(0)
    await_sends(1)
    await_sum(1)
    sums_ref[...] = whole[1]


def whiten(vertex_count, hidden_ref, inverse_ref, sums_ref, out_ref, loss_ref, result, sems):
    rows = hidden_ref.shape[0]
    across = (((1,), (1,)), ((), ()))
    step = rows // CHUNKS
    stores = []
    inverse = inverse_ref[...]
    high_part = inverse.astype(jnp.bfloat16)
    low_part = (inverse - high_part.astype(jnp.float32)).astype(jnp.bfloat16)
    for chunk in range(CHUNKS):
        here = pl.ds(chunk * step, step)
        hidden = hidden_ref[here, :]
        white = lax.dot_general(
            hidden, high_part, across, preferred_element_type=jnp.float32
        ) + lax.dot_general(hidden, low_part, across, preferred_element_type=jnp.float32)
        result[here, :] = white.astype(jnp.bfloat16)
        store = pltpu.make_async_copy(result.at[here], out_ref.at[here], sems.at[chunk])
        store.start()
        stores.append(store)
    feat = hidden_ref.shape[1]
    tops, sides, pair_at, side_at, extra_at = layout(feat)
    squares = extra_at + feat // 256
    row = lax.broadcasted_iota(jnp.int32, (128, 128), 0)
    lane = lax.broadcasted_iota(jnp.int32, (128, 128), 1)
    cross = jnp.zeros((128, 128), jnp.float32)
    norm = jnp.zeros((128, 128), jnp.float32)
    for top in tops:
        upper = inverse_ref[top : top + 128, top : top + 128]
        lower = inverse_ref[top + 128 : top + 256, top + 128 : top + 256]
        place = extra_at + top // 256
        pair = sums_ref[pair_at[top] : pair_at[top] + 128, :]
        low_diagonal = sums_ref[place : place + 1, :]
        cross = cross + jnp.where(row >= lane, upper, lower.T) * pair
        cross = cross + jnp.where(row == lane, lower * low_diagonal, 0.0)
        norm = norm + upper * upper + lower * lower
    for top, side in sides:
        at = side_at[top, side]
        across_block = inverse_ref[side : side + 128, top : top + 128]
        cross = cross + across_block * sums_ref[at : at + 128, :]
        norm = norm + across_block * across_block
    rest = jnp.sum(-2.0 * cross - (vertex_count * epsilon) * norm, axis=0, keepdims=True)
    rest = rest + sums_ref[squares : squares + 1, :]
    loss_ref[0, 0] = 1.0 + jnp.sum(rest) / (vertex_count * feat)
    for store in stores:
        store.wait()


def body(
    n_dom,
    n_sub,
    features,
    weight,
    send_far,
    send_near,
    tile_dst,
    inner_src,
    outer_src,
    tile_live,
    tile_weight,
):
    rows, feat = features.shape
    size = tile_weight.shape[1]
    slots = inner_src.shape[0]
    total = n_dom * n_sub
    wide = feat // 128
    extra = feat // 256 + 1
    packed_rows = feat // 2 + 64 * wide * (wide - 1) + extra
    share = 8
    while -(-packed_rows // share) > total // 2 + 1:
        share += 8
    packed_rows = -(-packed_rows // share) * share
    far_count = send_far.shape[0]
    near_count = send_near.shape[0]

    def padded(index, peers):
        each = index.shape[0] // peers
        grid = index.reshape(peers, each)
        return jnp.pad(grid, ((0, 0), (0, padded_rows(each) - each))).reshape(1, -1)

    far_index = padded(send_far, n_dom)
    near_index = padded(send_near, n_sub)
    far_padded = far_index.shape[1]
    near_padded = near_index.shape[1]
    anywhere = pl.BlockSpec(memory_space=pltpu.HBM)
    smem = pl.BlockSpec(memory_space=pltpu.SMEM)
    f32 = jnp.float32
    bf16 = jnp.bfloat16
    vmem = pl.BlockSpec(memory_space=pltpu.VMEM)
    hidden, inverse, sums = pl.pallas_call(
        functools.partial(kernel, n_dom, n_sub, near_count // n_sub),
        out_shape=(
            pltpu.VMEM((rows, feat), bf16),
            pltpu.VMEM((feat, feat), f32),
            pltpu.VMEM((packed_rows, 128), f32),
        ),
        in_specs=[anywhere] * 9,
        out_specs=(vmem, vmem, vmem),
        scratch_shapes=[
            pltpu.VMEM((rows // size, size, feat), bf16),
            pltpu.VMEM(weight.shape, bf16),
            pltpu.VMEM((1, far_padded), jnp.int32),
            pltpu.VMEM((1, near_padded), jnp.int32),
            pltpu.SMEM(tile_dst.shape, jnp.int32),
            pltpu.SMEM(inner_src.shape, jnp.int32),
            pltpu.SMEM(outer_src.shape, jnp.int32),
            pltpu.SMEM(tile_live.shape, jnp.int32),
            pltpu.VMEM(tile_weight.shape, bf16),
            pltpu.VMEM((far_padded, feat), bf16),
            pltpu.VMEM((near_padded, feat), bf16),
            pltpu.VMEM((far_padded + near_padded, feat), bf16),
            pltpu.VMEM(((far_count + near_count) // size, size, feat), bf16),
            pltpu.VMEM((slots, size, feat), f32),
            pltpu.VMEM((rows // size, size, feat), f32),
            pltpu.VMEM((rows, feat), bf16),
            pltpu.VMEM((feat, rows), bf16),
            pltpu.VMEM((2, packed_rows, 128), f32),
            pltpu.VMEM((2, total, share, 128), f32),
            pltpu.VMEM((2, share, 128), f32),
            pltpu.VMEM((2, packed_rows, 128), f32),
            pltpu.VMEM((feat, 2 * feat), f32),
            pltpu.SemaphoreType.DMA((10,)),
            pltpu.SemaphoreType.DMA((4,)),
            pltpu.SemaphoreType.DMA((8,)),
        ],
        compiler_params=pltpu.CompilerParams(
            collective_id=0, has_side_effects=True, vmem_limit_bytes=VMEM_LIMIT
        ),
    )(
        *[
            pltpu.with_memory_space_constraint(value, pltpu.HBM)
            for value in (
                features.reshape(rows // size, size, feat),
                weight,
                far_index,
                near_index,
                tile_dst,
                inner_src,
                outer_src,
                tile_live,
                tile_weight,
            )
        ]
    )
    whitened, loss = pl.pallas_call(
        functools.partial(whiten, rows * total),
        out_shape=(
            jax.ShapeDtypeStruct((rows, feat), bf16),
            jax.ShapeDtypeStruct((1, 1), f32),
        ),
        in_specs=[vmem, vmem, vmem],
        out_specs=(anywhere, smem),
        scratch_shapes=[pltpu.VMEM((rows, feat), bf16), pltpu.SemaphoreType.DMA((CHUNKS,))],
        compiler_params=pltpu.CompilerParams(vmem_limit_bytes=VMEM_LIMIT),
    )(hidden, inverse, sums)
    return whitened, loss.reshape(())


def solution(mesh):
    placed = (
        P(("dom", "sub"), None),
        P(),
        P(("dom", "sub")),
        P(("dom", "sub")),
        P(("dom", "sub")),
        P(("dom", "sub")),
        P(("dom", "sub")),
        P(("dom", "sub"), None),
        P(("dom", "sub"), None, None),
    )
    return jax.shard_map(
        functools.partial(body, mesh.shape["dom"], mesh.shape["sub"]),
        mesh=mesh,
        in_specs=placed,
        out_specs=(P(("dom", "sub"), None), P()),
        check_vma=False,
    )
```
